32 devices in a mesh: cuts: 8 (over y, x, core), grp: 4 (over z).
Axes of the slice: x: 2, y: 2, z: 4, core: 2. Of those that a mesh axis runs over, the one named last changes fastest.
Arguments:
- boundary: float32 [32, 2, 32, 32, 32], P('grp'), may hold values from -12 to 12
- gate_stack: float32 [3, 2, 1024, 1024], P(None, None, 'cuts'), may hold values from -0.125 to 0.125
- layer_order: int32 [3], replicated, may hold values from 0 to 2, each once
- cut_index: int32 [6, 3], replicated, may hold values from 0 to 4, as said below
- slice_bits: int32 [8, 6], P('cuts'), may hold values 0 or 1
- bitstrings: int32 [64, 20], replicated, may hold values 0 or 1
Outputs:
- amplitudes: float32 [64, 2], replicated
The draws below stay inside these ranges and needn't reach their ends.
Inputs may be any that keep to these rules, and one draw needn't show every extreme that they name: Each row of cut_index is (layer 0 to 2, group 0 to 3, bit 0 to 4); no two rows are equal. Rows of slice_bits need not differ.
All inputs are finite; a program needn't handle non-finite values.
Results may differ from the reference program's by a relative error of at most 0.0003.
Values sent between devices are 32-bit elements.
A program may use at most 320 MiB of HBM per device.

```python
import jax
import jax.numpy as jnp
from jax import lax

GROUP_BITS = 5
GROUP = 32
PAIR = 1024
QUBITS = 20
LAYERS = 3
CUT_COUNT = 6
BITSTRINGS = 64
SLICES = 8


def draw_cut_index(key, part):
    per_layer = 4 * GROUP_BITS
    pool_size = LAYERS * per_layer
    chosen = jax.random.permutation(key, pool_size)[:CUT_COUNT].astype(jnp.int32)
    layer_part = chosen // per_layer
    group_part = chosen % per_layer // GROUP_BITS
    bit_part = chosen % GROUP_BITS
    return jnp.stack((layer_part, group_part, bit_part), axis=1).astype(jnp.int32)


def set_ends(array, key, smallest, high):
    longest = array.shape.index(max(array.shape))
    spots = []
    for shift in (0, 1):
        where = [jax.random.randint(jax.random.fold_in(key, axis), (), 0, length) for axis, length in enumerate(array.shape)]
        where[longest] = (where[longest] + shift) % array.shape[longest]
        spots.append(tuple(where))
    return array.at[spots[0]].set(smallest).at[spots[1]].set(high)


def steps_of(own_key, shape, pieces, low, largest):
    gain, own = 1.0, jax.random.fold_in(own_key, 6)
    for dim, shards_of in pieces:
        steps = jnp.exp(jax.random.uniform(jax.random.fold_in(own, dim), (shards_of,), jnp.float32, low / len(pieces), largest / len(pieces)))
        gain = gain * jnp.repeat(steps, shape[dim] // shards_of).reshape([-1 if axis == dim else 1 for axis in range(len(shape))])
    return gain


def gaussian(rng, shape, spread, reach, shards=(), kind=jnp.bfloat16):
    array = spread * jax.random.normal(rng, shape, jnp.float32)
    if shards:
        array = array * steps_of(rng, shape, shards, -0.22, 0.18)
    return jnp.clip(array, -reach, reach).astype(kind)


def setup_inputs(seed: int = 0) -> dict:
    keys = jax.random.split(jax.random.key(seed), 7)
    return {
        "boundary": gaussian(keys[0], (GROUP, 2, GROUP, GROUP, GROUP), 2.0, 12.0, ((0, 4),), jnp.float32),
        "gate_stack": gaussian(keys[1], (LAYERS, 2, PAIR, PAIR), (2 * PAIR) ** -0.5, 0.125, ((2, 8),), jnp.float32),
        "layer_order": jax.random.permutation(keys[2], LAYERS).astype(jnp.int32),
        "cut_index": draw_cut_index(jax.random.fold_in(keys[6], 71), 0),
        "slice_bits": set_ends((jax.random.randint(keys[4], (SLICES, CUT_COUNT), 0, 2) < 1).astype(jnp.int32), jax.random.fold_in(keys[4], 1), 0, 1),
        "bitstrings": set_ends((jax.random.randint(keys[5], (BITSTRINGS, QUBITS), 0, 2) < 1).astype(jnp.int32), jax.random.fold_in(keys[5], 1), 0, 1),
    }


LAYER_KINDS = (0, 1, 2, 3, 2, 3, 0, 1)
PAIR_GROUPS = ((0, 1), (2, 3), (1, 2), (1, 3))
FULL_PRECISION = lax.Precision.HIGHEST


def slice_factors(cut_index, slice_bits, layer_id, group_id, extent, offset):
    positions = offset + jnp.arange(extent, dtype=jnp.int32)
    active = jnp.logical_and(cut_index[:, 0] == layer_id, cut_index[:, 1] == group_id)
    bit_values = jnp.right_shift(positions[:, None], cut_index[None, :, 2]) & 1
    agrees = bit_values[None, :, :] == slice_bits[:, None, :]
    kept = jnp.logical_or(agrees, jnp.logical_not(active)[None, None, :])
    return jnp.all(kept, axis=2).astype(jnp.float32)


def group_digits(bitstrings, group_bits):
    weights = jnp.left_shift(jnp.ones((group_bits,), jnp.int32), jnp.arange(group_bits, dtype=jnp.int32))
    return [jnp.sum(bitstrings[:, group_id * group_bits:(group_id + 1) * group_bits] * weights, axis=1).astype(jnp.int32) for group_id in range(4)]


def apply_gate(current, layer_gate, first_group, second_group):
    aligned = jnp.moveaxis(current, (1 + first_group, 1 + second_group), (1, 2))
    full_shape = aligned.shape
    matrix = aligned.reshape(2, full_shape[1] * full_shape[2], -1)
    real_part = jnp.dot(layer_gate[0], matrix[0], precision=FULL_PRECISION, preferred_element_type=jnp.float32) - jnp.dot(layer_gate[1], matrix[1], precision=FULL_PRECISION, preferred_element_type=jnp.float32)
    imag_part = jnp.dot(layer_gate[0], matrix[1], precision=FULL_PRECISION, preferred_element_type=jnp.float32) + jnp.dot(layer_gate[1], matrix[0], precision=FULL_PRECISION, preferred_element_type=jnp.float32)
    updated = jnp.stack((real_part, imag_part)).reshape(full_shape)
    return jnp.moveaxis(updated, (1, 2), (1 + first_group, 1 + second_group))


def reference(boundary, gate_stack, layer_order, cut_index, slice_bits, bitstrings):
    initial = jnp.moveaxis(boundary, 1, 0)
    digits = group_digits(bitstrings, GROUP_BITS)

    def add_slice(running, bits_row):
        current = initial
        for layer_id in range(LAYERS):
            first_group, second_group = PAIR_GROUPS[LAYER_KINDS[layer_id % 8]]
            layer_gate = gate_stack[layer_order[layer_id]]
            current = apply_gate(current, layer_gate, first_group, second_group)
            for group_id in range(4):
                factor = slice_factors(cut_index, bits_row[None, :], layer_id, group_id, GROUP, 0)[0]
                target_shape = tuple(GROUP if position == 1 + group_id else 1 for position in range(5))
                current = current * factor.reshape(target_shape)
        amplitude = current[:, digits[0], digits[1], digits[2], digits[3]]
        return running + amplitude.T, None

    running, leftover = lax.scan(add_slice, jnp.zeros((BITSTRINGS, 2), jnp.float32), slice_bits)
    return running
```

```python
import jax
import jax.numpy as jnp
from jax import lax
from jax.sharding import PartitionSpec as P

LAYER_KINDS = (0, 1, 2, 3, 2, 3, 0, 1)
PAIR_GROUPS = ((0, 1), (2, 3), (1, 2), (1, 3))
PRECISION = lax.Precision.HIGH


def keep_mask(cut_index, slice_bits, layers, group_id, positions):
    hit = cut_index[:, 1] == group_id
    active = jnp.zeros_like(hit)
    for layer_id in layers:
        active = jnp.logical_or(active, cut_index[:, 0] == layer_id)
    active = jnp.logical_and(active, hit)
    bit_values = jnp.right_shift(positions[:, None], cut_index[None, :, 2]) & 1
    agrees = bit_values[None, :, :] == slice_bits[:, None, :]
    kept = jnp.logical_or(agrees, jnp.logical_not(active)[None, None, :])
    return jnp.all(kept, axis=2).astype(jnp.float32)


def group_digits(bitstrings):
    bits = bitstrings.shape[1] // 4
    weights = jnp.left_shift(jnp.ones((bits,), jnp.int32), jnp.arange(bits, dtype=jnp.int32))
    return [
        jnp.sum(bitstrings[:, k * bits : (k + 1) * bits] * weights, axis=1).astype(jnp.int32)
        for k in range(4)
    ]


def dot(a, b):
    return jnp.dot(a, b, precision=PRECISION, preferred_element_type=jnp.float32)


def make_body(cuts, grps):

    def body(boundary, gate_stack, layer_order, cut_index, slice_bits, bitstrings):
        c = lax.axis_index("cuts")
        m = lax.axis_index("grp")
        n0, _, ext = boundary.shape[:3]
        pair = ext * ext
        rows = gate_stack.shape[2]
        kdim = n0 * ext
        cols = pair // grps
        local_slices = slice_bits.shape[0]
        g = group_digits(bitstrings)
        count = bitstrings.shape[0]

        gate0 = lax.dynamic_index_in_dim(gate_stack, layer_order[0], 0, keepdims=False)
        gate0 = lax.dynamic_slice_in_dim(gate0, m * kdim, kdim, 2)
        start = jnp.moveaxis(boundary, 1, 0).reshape(2, kdim, pair)
        phi = jnp.stack((
            dot(gate0[0], start[0]) - dot(gate0[1], start[1]),
            dot(gate0[0], start[1]) + dot(gate0[1], start[0]),
        ))
        phi = lax.psum_scatter(phi, "grp", scatter_dimension=2, tiled=True)

        gate1 = lax.dynamic_index_in_dim(gate_stack, layer_order[1], 0, keepdims=False)
        gate1 = lax.dynamic_slice_in_dim(gate1, m * cols, cols, 2)
        gate1 = lax.all_gather(gate1, "cuts", axis=1, tiled=True)

        gate2 = lax.dynamic_index_in_dim(gate_stack, layer_order[2], 0, keepdims=False)
        wanted = g[1] * ext + g[2] - rows * c
        inside = jnp.logical_and(wanted >= 0, wanted < rows)
        picked = jnp.take(gate2, jnp.clip(wanted, 0, rows - 1), axis=1) * inside[None, :, None]
        if ext % cuts == 0:
            width, sub = ext // cuts, 1
            chunk = width * ext
            bits = jnp.zeros((2, cuts, local_slices, chunk), jnp.float32)
            bits = bits.at[:, :, :, : slice_bits.shape[1]].set(slice_bits.astype(jnp.float32))
            own = (jnp.arange(cuts) == c).astype(jnp.float32)
            bits = bits[:, :, None] * own[None, None, :, None, None]
            bits = bits.reshape(2, cuts, cuts * local_slices, chunk)
            bits = jnp.moveaxis(bits, 1, 2)
            packed = jnp.concatenate((picked.reshape(2, count, cuts, chunk), bits), axis=1)
            packed = lax.psum_scatter(packed, "cuts", scatter_dimension=2, tiled=True)[:, :, 0]
            gate2 = packed[:, :count].reshape(2, count, width, ext)
            slice_bits = packed[0, count:, : slice_bits.shape[1]].astype(jnp.int32)
            phi = phi.reshape(2, rows // ext, ext, cols)
            phi = lax.all_to_all(phi, "cuts", split_axis=2, concat_axis=1, tiled=True)
        else:
            width, sub = 1, cuts // ext
            slice_bits = lax.all_gather(slice_bits, "cuts", axis=0, tiled=True)
            picked = lax.psum(picked, "cuts").reshape(2, count, ext, ext)
            gate2 = lax.dynamic_slice_in_dim(picked, c // sub, 1, 2)
            phi = lax.all_gather(phi, "cuts", axis=1, tiled=True).reshape(2, ext, ext, cols)
            phi = lax.dynamic_slice_in_dim(phi, c // sub, 1, 2)
        first_i1 = c // sub * width
        cols = cols // sub
        first_col = (m * sub + c % sub) * cols
        if sub > 1:
            phi = lax.dynamic_slice_in_dim(phi, c % sub * cols, cols, 3)
            gate1 = lax.dynamic_slice_in_dim(gate1, c % sub * cols, cols, 2)

        slices = slice_bits.shape[0]
        column = first_col + jnp.arange(cols, dtype=jnp.int32)
        last = jnp.ones((slices, count), jnp.float32)
        for group_id, layers in ((0, (0, 1, 2)), (1, (2,)), (2, (2,)), (3, (1, 2))):
            last = last * keep_mask(cut_index, slice_bits, layers, group_id, g[group_id])
        on_i1 = keep_mask(
            cut_index, slice_bits, (0, 1), 1, first_i1 + jnp.arange(width, dtype=jnp.int32)
        )
        on_i2 = keep_mask(cut_index, slice_bits, (1,), 2, jnp.arange(ext, dtype=jnp.int32))
        on_j = keep_mask(cut_index, slice_bits, (0,), 2, column // ext)
        on_j = on_j * keep_mask(cut_index, slice_bits, (0,), 3, column % ext)

        left = gate2[:, :, None] * on_i2[None, None, :, None, :]
        left_re = jnp.concatenate((left[0], -left[1]), axis=3)
        left_im = jnp.concatenate((left[1], left[0]), axis=3)
        left = jnp.stack((left_re, left_im), axis=1)
        left = left.reshape(count, 2 * slices * width, 2 * ext)
        right = gate1.reshape(2, ext, ext, cols)
        right = jnp.take(jnp.moveaxis(right, 2, 0).reshape(ext, 2 * ext, cols), g[3], axis=0)
        w = lax.dot_general(
            left, right, (((2,), (1,)), ((0,), (0,))),
            precision=PRECISION, preferred_element_type=jnp.float32,
        )
        w = w.reshape(count, 2, slices, width, cols)
        scale = last.T[:, :, None, None] * on_i1[None, :, :, None] * on_j[None, :, None, :]
        w = jnp.sum(w * scale[:, None], axis=2)
        psi = jnp.take(phi, g[0], axis=1)
        real = jnp.sum(w[:, 0] * psi[0] - w[:, 1] * psi[1], axis=(1, 2))
        imag = jnp.sum(w[:, 0] * psi[1] + w[:, 1] * psi[0], axis=(1, 2))
        return lax.psum(jnp.stack((real, imag), axis=1), ("cuts", "grp"))

    return body


def solution(mesh):
    return jax.shard_map(
        make_body(mesh.shape["cuts"], mesh.shape["grp"]),
        mesh=mesh,
        in_specs=(
            P("grp", None, None, None, None),
            P(None, None, "cuts", None),
            P(),
            P(),
            P("cuts", None),
            P(),
        ),
        out_specs=P(),
        check_vma=False,
    )
```

```python
import functools

import jax
import jax.numpy as jnp
from jax import lax
from jax.experimental import pallas as pl
from jax.experimental.pallas import tpu as pltpu
from jax.sharding import PartitionSpec as P

LAYER_KINDS = (0, 1, 2, 3, 2, 3, 0, 1)
PAIR_GROUPS = ((0, 1), (2, 3), (1, 2), (1, 3))
PRECISION = lax.Precision.HIGH


def keep_mask(cut_index, slice_bits, layers, group_id, positions):
    hit = cut_index[:, 1] == group_id
    active = jnp.zeros_like(hit)
    for layer_id in layers:
        active = jnp.logical_or(active, cut_index[:, 0] == layer_id)
    active = jnp.logical_and(active, hit)
    bit_values = jnp.right_shift(positions[:, None], cut_index[None, :, 2]) & 1
    agrees = bit_values[None, :, :] == slice_bits[:, None, :]
    kept = jnp.logical_or(agrees, jnp.logical_not(active)[None, None, :])
    return jnp.all(kept, axis=2).astype(jnp.float32)


def group_digits(bitstrings):
    bits = bitstrings.shape[1] // 4
    weights = jnp.left_shift(jnp.ones((bits,), jnp.int32), jnp.arange(bits, dtype=jnp.int32))
    return [
        jnp.sum(bitstrings[:, k * bits : (k + 1) * bits] * weights, axis=1).astype(jnp.int32)
        for k in range(4)
    ]


def dot(a, b):
    return jnp.dot(a, b, precision=PRECISION, preferred_element_type=jnp.float32)


def make_body(cuts, grps):

    def body(boundary, gate_stack, layer_order, cut_index, slice_bits, bitstrings):
        c = lax.axis_index("cuts")
        m = lax.axis_index("grp")
        n0, _, ext = boundary.shape[:3]
        pair = ext * ext
        rows = gate_stack.shape[2]
        kdim = n0 * ext
        cols = pair // grps
        local_slices = slice_bits.shape[0]
        g = group_digits(bitstrings)
        count = bitstrings.shape[0]

        gate0 = lax.dynamic_index_in_dim(gate_stack, layer_order[0], 0, keepdims=False)
        gate0 = lax.dynamic_slice_in_dim(gate0, m * kdim, kdim, 2)
        start = jnp.moveaxis(boundary, 1, 0).reshape(2, kdim, pair)
        phi = jnp.stack((
            dot(gate0[0], start[0]) - dot(gate0[1], start[1]),
            dot(gate0[0], start[1]) + dot(gate0[1], start[0]),
        ))
        phi = lax.psum_scatter(phi, "grp", scatter_dimension=2, tiled=True)

        gate1 = lax.dynamic_index_in_dim(gate_stack, layer_order[1], 0, keepdims=False)
        gate1 = lax.dynamic_slice_in_dim(gate1, m * cols, cols, 2)
        gate1 = lax.all_gather(gate1, "cuts", axis=1, tiled=True)

        gate2 = lax.dynamic_index_in_dim(gate_stack, layer_order[2], 0, keepdims=False)
        wanted = g[1] * ext + g[2] - rows * c
        inside = jnp.logical_and(wanted >= 0, wanted < rows)
        picked = jnp.take(gate2, jnp.clip(wanted, 0, rows - 1), axis=1) * inside[None, :, None]
        if ext % cuts == 0:
            width, sub = ext // cuts, 1
            chunk = width * ext
            bits = jnp.zeros((2, cuts, local_slices, chunk), jnp.float32)
            bits = bits.at[:, :, :, : slice_bits.shape[1]].set(slice_bits.astype(jnp.float32))
            own = (jnp.arange(cuts) == c).astype(jnp.float32)
            bits = bits[:, :, None] * own[None, None, :, None, None]
            bits = bits.reshape(2, cuts, cuts * local_slices, chunk)
            bits = jnp.moveaxis(bits, 1, 2)
            packed = jnp.concatenate((picked.reshape(2, count, cuts, chunk), bits), axis=1)
            packed = lax.psum_scatter(packed, "cuts", scatter_dimension=2, tiled=True)[:, :, 0]
            gate2 = packed[:, :count].reshape(2, count, width, ext)
            slice_bits = packed[0, count:, : slice_bits.shape[1]].astype(jnp.int32)
            phi = phi.reshape(2, rows // ext, ext, cols)
            phi = lax.all_to_all(phi, "cuts", split_axis=2, concat_axis=1, tiled=True)
        else:
            width, sub = 1, cuts // ext
            slice_bits = lax.all_gather(slice_bits, "cuts", axis=0, tiled=True)
            picked = lax.psum(picked, "cuts").reshape(2, count, ext, ext)
            gate2 = lax.dynamic_slice_in_dim(picked, c // sub, 1, 2)
            phi = lax.all_gather(phi, "cuts", axis=1, tiled=True).reshape(2, ext, ext, cols)
            phi = lax.dynamic_slice_in_dim(phi, c // sub, 1, 2)
        first_i1 = c // sub * width
        cols = cols // sub
        first_col = (m * sub + c % sub) * cols
        if sub > 1:
            phi = lax.dynamic_slice_in_dim(phi, c % sub * cols, cols, 3)
            gate1 = lax.dynamic_slice_in_dim(gate1, c % sub * cols, cols, 2)

        slices = slice_bits.shape[0]
        column = first_col + jnp.arange(cols, dtype=jnp.int32)
        last = jnp.ones((slices, count), jnp.float32)
        for group_id, layers in ((0, (0, 1, 2)), (1, (2,)), (2, (2,)), (3, (1, 2))):
            last = last * keep_mask(cut_index, slice_bits, layers, group_id, g[group_id])
        on_i1 = keep_mask(
            cut_index, slice_bits, (0, 1), 1, first_i1 + jnp.arange(width, dtype=jnp.int32)
        )
        on_i2 = keep_mask(cut_index, slice_bits, (1,), 2, jnp.arange(ext, dtype=jnp.int32))
        on_j = keep_mask(cut_index, slice_bits, (0,), 2, column // ext)
        on_j = on_j * keep_mask(cut_index, slice_bits, (0,), 3, column % ext)

        left = gate2[:, :, None] * on_i2[None, None, :, None, :]
        left_re = jnp.concatenate((left[0], -left[1]), axis=3)
        left_im = jnp.concatenate((left[1], left[0]), axis=3)
        left = jnp.stack((left_re, left_im), axis=1)
        left = left.reshape(count, 2 * slices * width, 2 * ext)
        right = gate1.reshape(2, ext, ext, cols)
        right = jnp.take(jnp.moveaxis(right, 2, 0).reshape(ext, 2 * ext, cols), g[3], axis=0)
        w = lax.dot_general(
            left, right, (((2,), (1,)), ((0,), (0,))),
            precision=PRECISION, preferred_element_type=jnp.float32,
        )
        w = w.reshape(count, 2, slices, width, cols)
        scale = last.T[:, :, None, None] * on_i1[None, :, :, None] * on_j[None, :, None, :]
        w = jnp.sum(w * scale[:, None], axis=2)
        psi = jnp.take(phi, g[0], axis=1)
        real = jnp.sum(w[:, 0] * psi[0] - w[:, 1] * psi[1], axis=(1, 2))
        imag = jnp.sum(w[:, 0] * psi[1] + w[:, 1] * psi[0], axis=(1, 2))
        return lax.psum(jnp.stack((real, imag), axis=1), ("cuts", "grp"))

    return body


VMEM = pl.BlockSpec(memory_space=pltpu.VMEM)
HI = lax.Precision.HIGHEST


def split(x):
    hi = lax.reduce_precision(x, 8, 7)
    return hi.astype(jnp.bfloat16), (x - hi).astype(jnp.bfloat16)


def flip(index, step):
    return index + step * (1 - 2 * ((index // step) % 2))


def greet(cuts, grps):
    c, m = lax.axis_index("cuts"), lax.axis_index("grp")
    barrier = pltpu.get_barrier_semaphore()
    for d in range(1, cuts):
        pl.semaphore_signal(barrier, inc=1, device_id={"cuts": (c + d) % cuts})
    for d in range(1, grps):
        pl.semaphore_signal(barrier, inc=1, device_id={"grp": (m + d) % grps})
    pl.semaphore_wait(barrier, cuts + grps - 2)
    return c, m


def exchange_kernel(
    cuts, grps, lh, ll, bh, bl, u1, packed, u1_all, phi_out, u2_out,
    parts, landed, phis, u2_in,
    u_send, u_recv, r_send, r_recv, p_send, p_recv, k_send, k_recv, own_sem,
):
    c, m = greet(cuts, grps)
    core, east, north = flip(c, 1), flip(c, 2), flip(c, 4)
    half = u1.shape[0] // 2
    low, high = pl.ds(0, half), pl.ds(half, half)

    def send_u1(slot, src, dst, target):
        return pltpu.make_async_remote_copy(
            src_ref=src, dst_ref=dst, send_sem=u_send.at[slot], recv_sem=u_recv.at[slot],
            device_id={"cuts": target},
        )

    own = pltpu.make_async_copy(u1, u1_all.at[c], own_sem)
    own.start()
    east_low = send_u1(0, u1.at[low], u1_all.at[c, low], east)
    north_high = send_u1(1, u1.at[high], u1_all.at[c, high], north)
    east_high = send_u1(2, u1.at[high], u1_all.at[c, high], east)
    north_low = send_u1(3, u1.at[low], u1_all.at[c, low], north)
    to_core = send_u1(4, u1, u1_all.at[c], core)
    for copy in (east_low, north_high, east_high, north_low, to_core):
        copy.start()

    row_copies = []
    for d in range(1, cuts):
        to = (c + d) % cuts
        copy = pltpu.make_async_remote_copy(
            src_ref=packed.at[to], dst_ref=u2_in.at[d - 1],
            send_sem=k_send.at[d - 1], recv_sem=k_recv.at[d - 1], device_id={"cuts": to},
        )
        row_copies.append(copy)

    cols = parts.shape[2]

    def product(part):
        at = pl.ds(pl.multiple_of(part * cols, cols), cols)
        bhi, blo = bh[:, at], bl[:, at]
        mm = functools.partial(jnp.dot, preferred_element_type=jnp.float32)
        return mm(lh[...], bhi) + (mm(lh[...], blo) + mm(ll[...], bhi))

    sums = {}
    for d in sorted(range(1, grps), key=lambda d: -min(d, grps - d)):
        to = (m + d) % grps
        parts[d - 1] = product(to)
        sums[d] = pltpu.make_async_remote_copy(
            src_ref=parts.at[d - 1], dst_ref=landed.at[d - 1],
            send_sem=r_send.at[d - 1], recv_sem=r_recv.at[d - 1], device_id={"grp": to},
        )
        sums[d].start()
    total = product(m)

    east_low.wait_recv()
    on_north = send_u1(5, u1_all.at[east, low], u1_all.at[east, low], north)
    on_north.start()
    north_high.wait_recv()
    on_east = send_u1(6, u1_all.at[north, high], u1_all.at[north, high], east)
    on_east.start()
    for copy in row_copies:
        copy.start()
    east_high.wait_recv()
    core_east = send_u1(7, u1_all.at[east], u1_all.at[east], core)
    core_east.start()
    north_low.wait_recv()
    core_north = send_u1(8, u1_all.at[north], u1_all.at[north], core)
    core_north.start()
    on_north.wait_recv()
    on_east.wait_recv()
    far = flip(east, 4)
    core_far = send_u1(9, u1_all.at[far], u1_all.at[far], core)
    core_far.start()

    for d in range(1, grps):
        sums[d].wait_recv()
        total = total + landed[d - 1]
    phis[...] = total.reshape(phis.shape)
    phi_out[c] = phis[c]
    turned = []
    for d in range(1, cuts):
        to = (c + d) % cuts
        copy = pltpu.make_async_remote_copy(
            src_ref=phis.at[to], dst_ref=phi_out.at[c],
            send_sem=p_send.at[d - 1], recv_sem=p_recv.at[d - 1], device_id={"cuts": to},
        )
        copy.start()
        turned.append(copy)

    rows = packed[c]
    for d in range(1, cuts):
        row_copies[d - 1].wait_recv()
        rows = rows + u2_in[d - 1]
    u2_out[...] = rows
    for copy in (to_core, core_east, core_north, core_far):
        copy.wait_recv()
    for copy in turned:
        copy.wait_recv()
    own.wait()
    for copy in (
        east_low, north_high, east_high, north_low, to_core, on_north, on_east,
        core_east, core_north, core_far, *row_copies, *sums.values(), *turned,
    ):
        copy.wait_send()


def finish_kernel(
    cuts, grps, g0, g3, left, u1_all, phi, on_j, out,
    acc, mine, from_grp, mid, from_cuts, g_send, g_recv, c_send, c_recv,
):
    c, m = greet(cuts, grps)
    count = left.shape[0]
    slices = on_j.shape[0]
    tile = phi.shape[1]
    lanes = 128
    row = lax.broadcasted_iota(jnp.int32, (tile, 1), 0)
    sign = jnp.where(row < tile // 2, 1.0, -1.0)

    def one(b, carry):
        block = u1_all[:, g3[b]]
        block = block.reshape(block.shape[0] * block.shape[1], block.shape[2])
        hi = block.astype(jnp.bfloat16)
        lo = (block - hi.astype(jnp.float32)).astype(jnp.bfloat16)
        right = jnp.concatenate((hi, hi, lo), axis=0)
        w = jnp.dot(left[b], right, preferred_element_type=jnp.float32)
        w = w.reshape(slices, tile, w.shape[1])
        w = jnp.sum(w * on_j[...][:, None, :], axis=0)
        psi = phi[g0[b]]
        turned = jnp.concatenate((psi[tile // 2 :], psi[: tile // 2]), axis=0)
        real = jnp.sum(w * psi * sign, axis=0, keepdims=True)
        imag = jnp.sum(w * turned, axis=0, keepdims=True)
        fold = lambda v: functools.reduce(
            lambda p, q: p + q, [v[:, k : k + lanes] for k in range(0, v.shape[1], lanes)]
        )
        acc[0, pl.ds(b, 1), :] = fold(real)
        acc[1, pl.ds(b, 1), :] = fold(imag)
        return carry

    lax.fori_loop(0, count, one, 0)
    ones = jnp.ones((8, lanes), jnp.float32)
    add = lambda v: lax.dot_general(
        ones, v, (((1,), (1,)), ((), ())), precision=HI, preferred_element_type=jnp.float32
    )
    mine[...] = jnp.where(
        lax.broadcasted_iota(jnp.int32, mine.shape, 0) == 0, add(acc[0]), add(acc[1])
    )

    def everyone(axis, me, size, src, slots, send, recv):
        slots[me] = src[...]
        copies = []
        for d in range(1, size):
            to = (me + d) % size
            copy = pltpu.make_async_remote_copy(
                src_ref=src, dst_ref=slots.at[me],
                send_sem=send.at[d - 1], recv_sem=recv.at[d - 1], device_id={axis: to},
            )
            copy.start()
            copies.append(copy)
        for copy in copies:
            copy.wait()
        return functools.reduce(lambda p, q: p + q, [slots[k] for k in range(size)])

    mid[...] = everyone("grp", m, grps, mine, from_grp, g_send, g_recv)
    out[...] = everyone("cuts", c, cuts, mid, from_cuts, c_send, c_recv)


def make_fast_body(cuts, grps):

    def body(boundary, gate_stack, layer_order, cut_index, slice_bits, bitstrings):
        c = lax.axis_index("cuts")
        m = lax.axis_index("grp")
        n0, _, ext = boundary.shape[:3]
        pair = ext * ext
        rows = gate_stack.shape[2]
        kdim = n0 * ext
        cols = pair // grps
        width = ext // cuts
        own_rows = rows // ext
        local_slices = slice_bits.shape[0]
        slices = cuts * local_slices
        g = group_digits(bitstrings)
        count = bitstrings.shape[0]
        chunk = width * ext
        f32 = jnp.float32

        gate0 = lax.dynamic_slice(gate_stack, (layer_order[0], 0, 0, m * kdim), (1, 2, rows, kdim))[0]
        big = jnp.stack((
            jnp.concatenate((gate0[0], -gate0[1]), axis=1),
            jnp.concatenate((gate0[1], gate0[0]), axis=1),
        ))
        big = big.reshape(2, own_rows, cuts, width, 2 * kdim)
        big = jnp.transpose(big, (2, 1, 0, 3, 4)).reshape(2 * rows, 2 * kdim)
        lh, ll = split(big)
        start = boundary.reshape(n0, 2, ext, pair)
        start = jnp.moveaxis(start, 1, 0).reshape(2 * kdim, pair)
        bh, bl = split(start)

        gate1 = lax.dynamic_slice(gate_stack, (layer_order[1], 0, 0, m * cols), (1, 2, rows, cols))[0]
        gate1 = jnp.transpose(gate1.reshape(2, own_rows, ext, cols), (2, 0, 1, 3))
        gate1 = gate1.reshape(ext, 2 * own_rows, cols)

        gate2 = lax.dynamic_index_in_dim(gate_stack, layer_order[2], 0, keepdims=False)
        wanted = g[1] * ext + g[2] - rows * c
        pick = (wanted[:, None] == jnp.arange(rows)[None, :]).astype(f32)
        picked = jnp.stack([jnp.dot(pick, gate2[k], precision=HI) for k in (0, 1)])
        picked = jnp.transpose(picked.reshape(2 * count, cuts, chunk), (1, 0, 2))
        extra = -(-slices // 8) * 8
        bits = jnp.zeros((local_slices, chunk), f32).at[:, : slice_bits.shape[1]].set(slice_bits.astype(f32))
        bits = lax.dynamic_update_slice(jnp.zeros((extra, chunk), f32), bits, (c * local_slices, 0))
        bits = jnp.broadcast_to(bits, (cuts, extra, chunk))
        packed = jnp.concatenate((picked, bits), axis=1)

        dma = pltpu.SemaphoreType.DMA
        u1_all, phi, u2 = pl.pallas_call(
            functools.partial(exchange_kernel, cuts, grps),
            out_shape=(
                jax.ShapeDtypeStruct((cuts,) + gate1.shape, f32),
                jax.ShapeDtypeStruct((cuts, 2 * rows // cuts, cols), f32),
                jax.ShapeDtypeStruct(packed.shape[1:], f32),
            ),
            in_specs=[VMEM] * 6,
            out_specs=(VMEM,) * 3,
            scratch_shapes=[
                pltpu.VMEM((grps - 1, 2 * rows, cols), f32),
                pltpu.VMEM((grps - 1, 2 * rows, cols), f32),
                pltpu.VMEM((cuts, 2 * rows // cuts, cols), f32),
                pltpu.VMEM((cuts - 1,) + packed.shape[1:], f32),
                dma((10,)), dma((10,)), dma((grps - 1,)), dma((grps - 1,)),
                dma((cuts - 1,)), dma((cuts - 1,)), dma((cuts - 1,)), dma((cuts - 1,)), dma,
            ],
            compiler_params=pltpu.CompilerParams(
                collective_id=0, has_side_effects=True, vmem_limit_bytes=48 << 20
            ),
            name="exchange",
        )(lh, ll, bh, bl, gate1, packed)

        slice_bits = u2[2 * count : 2 * count + slices, : slice_bits.shape[1]].astype(jnp.int32)
        gate2 = u2[: 2 * count].reshape(2, count, width, cuts, own_rows)

        first_i1 = c * width
        column = m * cols + jnp.arange(cols, dtype=jnp.int32)
        last = jnp.ones((slices, count), f32)
        for group_id, layers in ((0, (0, 1, 2)), (1, (2,)), (2, (2,)), (3, (1, 2))):
            last = last * keep_mask(cut_index, slice_bits, layers, group_id, g[group_id])
        on_i1 = keep_mask(
            cut_index, slice_bits, (0, 1), 1, first_i1 + jnp.arange(width, dtype=jnp.int32)
        )
        on_i2 = keep_mask(cut_index, slice_bits, (1,), 2, jnp.arange(ext, dtype=jnp.int32))
        on_i2 = on_i2.reshape(slices, cuts, own_rows)
        on_j = keep_mask(cut_index, slice_bits, (0,), 2, column // ext)
        on_j = on_j * keep_mask(cut_index, slice_bits, (0,), 3, column % ext)

        base = jnp.stack((
            jnp.stack((gate2[0], -gate2[1]), axis=3),
            jnp.stack((gate2[1], gate2[0]), axis=3),
        ), axis=1)
        scale = last.T[:, :, None] * on_i1[None]
        left = base[:, None] * scale[:, :, None, :, None, None, None]
        left = left * on_i2[None, :, None, None, :, None, :]
        left = left.reshape(count, slices * 2 * width, 2 * ext)
        hi, lo = split(left)
        left = jnp.concatenate((hi, lo, hi), axis=2)

        smem = pl.BlockSpec(memory_space=pltpu.SMEM)
        tile = (8, count)
        out = pl.pallas_call(
            functools.partial(finish_kernel, cuts, grps),
            out_shape=jax.ShapeDtypeStruct(tile, f32),
            in_specs=[smem, smem] + [VMEM] * 4,
            out_specs=VMEM,
            scratch_shapes=[
                pltpu.VMEM((2, count, 128), f32),
                pltpu.VMEM(tile, f32), pltpu.VMEM((grps,) + tile, f32),
                pltpu.VMEM(tile, f32), pltpu.VMEM((cuts,) + tile, f32),
                dma((grps - 1,)), dma((grps - 1,)), dma((cuts - 1,)), dma((cuts - 1,)),
            ],
            compiler_params=pltpu.CompilerParams(
                collective_id=1, has_side_effects=True, vmem_limit_bytes=48 << 20
            ),
            name="finish",
        )(g[0], g[3], left, u1_all, phi.reshape(ext, 2 * width, cols), on_j)
        return out[:2].T

    return body


def solution(mesh):
    fast = mesh.shape["cuts"] == 8
    maker = make_fast_body if fast else make_body
    return jax.shard_map(
        maker(mesh.shape["cuts"], mesh.shape["grp"]),
        mesh=mesh,
        in_specs=(
            P("grp", None, None, None, None),
            P(None, None, "cuts", None),
            P(),
            P(),
            P("cuts", None),
            P(),
        ),
        out_specs=P(),
        check_vma=False,
    )
```

```python
import functools

import jax
import jax.numpy as jnp
from jax import lax
from jax.experimental import pallas as pl
from jax.experimental.pallas import tpu as pltpu
from jax.sharding import PartitionSpec as P

LAYER_KINDS = (0, 1, 2, 3, 2, 3, 0, 1)
PAIR_GROUPS = ((0, 1), (2, 3), (1, 2), (1, 3))
PRECISION = lax.Precision.HIGH


def keep_mask(cut_index, slice_bits, layers, group_id, positions):
    hit = cut_index[:, 1] == group_id
    active = jnp.zeros_like(hit)
    for layer_id in layers:
        active = jnp.logical_or(active, cut_index[:, 0] == layer_id)
    active = jnp.logical_and(active, hit)
    bit_values = jnp.right_shift(positions[:, None], cut_index[None, :, 2]) & 1
    agrees = bit_values[None, :, :] == slice_bits[:, None, :]
    kept = jnp.logical_or(agrees, jnp.logical_not(active)[None, None, :])
    return jnp.all(kept, axis=2).astype(jnp.float32)


def group_digits(bitstrings):
    bits = bitstrings.shape[1] // 4
    weights = jnp.left_shift(jnp.ones((bits,), jnp.int32), jnp.arange(bits, dtype=jnp.int32))
    return [
        jnp.sum(bitstrings[:, k * bits : (k + 1) * bits] * weights, axis=1).astype(jnp.int32)
        for k in range(4)
    ]


def dot(a, b):
    return jnp.dot(a, b, precision=PRECISION, preferred_element_type=jnp.float32)


def make_body(cuts, grps):

    def body(boundary, gate_stack, layer_order, cut_index, slice_bits, bitstrings):
        c = lax.axis_index("cuts")
        m = lax.axis_index("grp")
        n0, _, ext = boundary.shape[:3]
        pair = ext * ext
        rows = gate_stack.shape[2]
        kdim = n0 * ext
        cols = pair // grps
        local_slices = slice_bits.shape[0]
        g = group_digits(bitstrings)
        count = bitstrings.shape[0]

        gate0 = lax.dynamic_index_in_dim(gate_stack, layer_order[0], 0, keepdims=False)
        gate0 = lax.dynamic_slice_in_dim(gate0, m * kdim, kdim, 2)
        start = jnp.moveaxis(boundary, 1, 0).reshape(2, kdim, pair)
        phi = jnp.stack((
            dot(gate0[0], start[0]) - dot(gate0[1], start[1]),
            dot(gate0[0], start[1]) + dot(gate0[1], start[0]),
        ))
        phi = lax.psum_scatter(phi, "grp", scatter_dimension=2, tiled=True)

        gate1 = lax.dynamic_index_in_dim(gate_stack, layer_order[1], 0, keepdims=False)
        gate1 = lax.dynamic_slice_in_dim(gate1, m * cols, cols, 2)
        gate1 = lax.all_gather(gate1, "cuts", axis=1, tiled=True)

        gate2 = lax.dynamic_index_in_dim(gate_stack, layer_order[2], 0, keepdims=False)
        wanted = g[1] * ext + g[2] - rows * c
        inside = jnp.logical_and(wanted >= 0, wanted < rows)
        picked = jnp.take(gate2, jnp.clip(wanted, 0, rows - 1), axis=1) * inside[None, :, None]
        if ext % cuts == 0:
            width, sub = ext // cuts, 1
            chunk = width * ext
            bits = jnp.zeros((2, cuts, local_slices, chunk), jnp.float32)
            bits = bits.at[:, :, :, : slice_bits.shape[1]].set(slice_bits.astype(jnp.float32))
            own = (jnp.arange(cuts) == c).astype(jnp.float32)
            bits = bits[:, :, None] * own[None, None, :, None, None]
            bits = bits.reshape(2, cuts, cuts * local_slices, chunk)
            bits = jnp.moveaxis(bits, 1, 2)
            packed = jnp.concatenate((picked.reshape(2, count, cuts, chunk), bits), axis=1)
            packed = lax.psum_scatter(packed, "cuts", scatter_dimension=2, tiled=True)[:, :, 0]
            gate2 = packed[:, :count].reshape(2, count, width, ext)
            slice_bits = packed[0, count:, : slice_bits.shape[1]].astype(jnp.int32)
            phi = phi.reshape(2, rows // ext, ext, cols)
            phi = lax.all_to_all(phi, "cuts", split_axis=2, concat_axis=1, tiled=True)
        else:
            width, sub = 1, cuts // ext
            slice_bits = lax.all_gather(slice_bits, "cuts", axis=0, tiled=True)
            picked = lax.psum(picked, "cuts").reshape(2, count, ext, ext)
            gate2 = lax.dynamic_slice_in_dim(picked, c // sub, 1, 2)
            phi = lax.all_gather(phi, "cuts", axis=1, tiled=True).reshape(2, ext, ext, cols)
            phi = lax.dynamic_slice_in_dim(phi, c // sub, 1, 2)
        first_i1 = c // sub * width
        cols = cols // sub
        first_col = (m * sub + c % sub) * cols
        if sub > 1:
            phi = lax.dynamic_slice_in_dim(phi, c % sub * cols, cols, 3)
            gate1 = lax.dynamic_slice_in_dim(gate1, c % sub * cols, cols, 2)

        slices = slice_bits.shape[0]
        column = first_col + jnp.arange(cols, dtype=jnp.int32)
        last = jnp.ones((slices, count), jnp.float32)
        for group_id, layers in ((0, (0, 1, 2)), (1, (2,)), (2, (2,)), (3, (1, 2))):
            last = last * keep_mask(cut_index, slice_bits, layers, group_id, g[group_id])
        on_i1 = keep_mask(
            cut_index, slice_bits, (0, 1), 1, first_i1 + jnp.arange(width, dtype=jnp.int32)
        )
        on_i2 = keep_mask(cut_index, slice_bits, (1,), 2, jnp.arange(ext, dtype=jnp.int32))
        on_j = keep_mask(cut_index, slice_bits, (0,), 2, column // ext)
        on_j = on_j * keep_mask(cut_index, slice_bits, (0,), 3, column % ext)

        left = gate2[:, :, None] * on_i2[None, None, :, None, :]
        left_re = jnp.concatenate((left[0], -left[1]), axis=3)
        left_im = jnp.concatenate((left[1], left[0]), axis=3)
        left = jnp.stack((left_re, left_im), axis=1)
        left = left.reshape(count, 2 * slices * width, 2 * ext)
        right = gate1.reshape(2, ext, ext, cols)
        right = jnp.take(jnp.moveaxis(right, 2, 0).reshape(ext, 2 * ext, cols), g[3], axis=0)
        w = lax.dot_general(
            left, right, (((2,), (1,)), ((0,), (0,))),
            precision=PRECISION, preferred_element_type=jnp.float32,
        )
        w = w.reshape(count, 2, slices, width, cols)
        scale = last.T[:, :, None, None] * on_i1[None, :, :, None] * on_j[None, :, None, :]
        w = jnp.sum(w * scale[:, None], axis=2)
        psi = jnp.take(phi, g[0], axis=1)
        real = jnp.sum(w[:, 0] * psi[0] - w[:, 1] * psi[1], axis=(1, 2))
        imag = jnp.sum(w[:, 0] * psi[1] + w[:, 1] * psi[0], axis=(1, 2))
        return lax.psum(jnp.stack((real, imag), axis=1), ("cuts", "grp"))

    return body


VMEM = pl.BlockSpec(memory_space=pltpu.VMEM)
HI = lax.Precision.HIGHEST


def split(x):
    hi = lax.reduce_precision(x, 8, 7)
    return hi.astype(jnp.bfloat16), (x - hi).astype(jnp.bfloat16)


def flip(index, step):
    return index + step * (1 - 2 * ((index // step) % 2))


def greet(cuts, grps):
    c, m = lax.axis_index("cuts"), lax.axis_index("grp")
    barrier = pltpu.get_barrier_semaphore()
    for d in range(1, cuts):
        pl.semaphore_signal(barrier, inc=1, device_id={"cuts": (c + d) % cuts})
    for d in range(1, grps):
        pl.semaphore_signal(barrier, inc=1, device_id={"grp": (m + d) % grps})
    pl.semaphore_wait(barrier, cuts + grps - 2)
    return c, m


def whole_kernel(
    cuts, grps, g0, g3, lh, ll, bh, bl, u1, packed, out,
    u1_all, phi, base, masks, weight, wt,
    parts, landed, phis, u2_in, acc, mine, from_grp, mid, from_cuts,
    u_send, u_recv, r_send, r_recv, p_send, p_recv, k_send, k_recv, own_sem,
    g_send, g_recv, c_send, c_recv,
):
    c, m = greet(cuts, grps)
    core, east, north = flip(c, 1), flip(c, 2), flip(c, 4)
    half = u1.shape[0] // 2
    low, high = pl.ds(0, half), pl.ds(half, half)

    def send_u1(slot, src, dst, target):
        return pltpu.make_async_remote_copy(
            src_ref=src, dst_ref=dst, send_sem=u_send.at[slot], recv_sem=u_recv.at[slot],
            device_id={"cuts": target},
        )

    own = pltpu.make_async_copy(u1, u1_all.at[c], own_sem)
    own.start()
    east_low = send_u1(0, u1.at[low], u1_all.at[c, low], east)
    north_high = send_u1(1, u1.at[high], u1_all.at[c, high], north)
    east_high = send_u1(2, u1.at[high], u1_all.at[c, high], east)
    north_low = send_u1(3, u1.at[low], u1_all.at[c, low], north)
    to_core = send_u1(4, u1, u1_all.at[c], core)
    for copy in (east_low, north_high, east_high, north_low, to_core):
        copy.start()

    row_copies = []
    for d in range(1, cuts):
        to = (c + d) % cuts
        copy = pltpu.make_async_remote_copy(
            src_ref=packed.at[to], dst_ref=u2_in.at[d - 1],
            send_sem=k_send.at[d - 1], recv_sem=k_recv.at[d - 1], device_id={"cuts": to},
        )
        row_copies.append(copy)

    cols = parts.shape[2]

    def product(part):
        at = pl.ds(pl.multiple_of(part * cols, cols), cols)
        bhi, blo = bh[:, at], bl[:, at]
        mm = functools.partial(jnp.dot, preferred_element_type=jnp.float32)
        return mm(lh[...], bhi) + (mm(lh[...], blo) + mm(ll[...], bhi))

    sums = {}
    for d in sorted(range(1, grps), key=lambda d: -min(d, grps - d)):
        to = (m + d) % grps
        parts[d - 1] = product(to)
        sums[d] = pltpu.make_async_remote_copy(
            src_ref=parts.at[d - 1], dst_ref=landed.at[d - 1],
            send_sem=r_send.at[d - 1], recv_sem=r_recv.at[d - 1], device_id={"grp": to},
        )
        sums[d].start()
    total = product(m)

    east_low.wait_recv()
    on_north = send_u1(5, u1_all.at[east, low], u1_all.at[east, low], north)
    on_north.start()
    north_high.wait_recv()
    on_east = send_u1(6, u1_all.at[north, high], u1_all.at[north, high], east)
    on_east.start()
    for copy in row_copies:
        copy.start()
    east_high.wait_recv()
    core_east = send_u1(7, u1_all.at[east], u1_all.at[east], core)
    core_east.start()
    north_low.wait_recv()
    core_north = send_u1(8, u1_all.at[north], u1_all.at[north], core)
    core_north.start()
    on_north.wait_recv()
    on_east.wait_recv()
    far = flip(east, 4)
    core_far = send_u1(9, u1_all.at[far], u1_all.at[far], core)
    core_far.start()


    lanes = packed.shape[2]
    tile = phi.shape[1]
    half_tile = tile // 2
    count = wt.shape[0]
    pairs = count // 2
    picked_rows = pairs * half_tile
    for d in range(1, cuts):
        row_copies[d - 1].wait_recv()
    rows = packed[c, pl.ds(0, picked_rows)]
    for d in range(1, cuts):
        rows = rows + u2_in[d - 1, pl.ds(0, picked_rows)]
    rows = rows.reshape(picked_rows // tile, tile, lanes)
    lane = lax.broadcasted_iota(jnp.int32, (1, 1, lanes), 2)
    row = lax.broadcasted_iota(jnp.int32, (1, tile, 1), 1)
    quarter = lanes // 4
    even = (lane // quarter) % 2 == 0
    real_rows = jnp.where(even, rows, -rows)
    imag_rows = jnp.where(even, pltpu.roll(rows, lanes - quarter, 2), pltpu.roll(rows, quarter, 2))
    upper = row < half_tile
    base[:, 0] = jnp.where(upper, real_rows, pltpu.roll(imag_rows, half_tile, 1))
    base[:, 1] = jnp.where(upper, pltpu.roll(real_rows, half_tile, 1), imag_rows)
    first = lax.broadcasted_iota(jnp.int32, (1, lanes), 1) < lanes // 2
    for s in range(cuts):
        slot = packed.at[c] if s == 0 else u2_in.at[s - 1]
        mask = slot[pl.ds(picked_rows, tile)]
        masks[0, s] = jnp.where(first, mask, 0.0)
        masks[1, s] = jnp.where(first, 0.0, mask)
        on_b = slot[pl.ds(picked_rows + tile, tile)]
        on_j = slot[pl.ds(picked_rows + 2 * tile, tile)]
        column = jnp.transpose(on_b)[:count, 0:1]
        weight[s] = column * jnp.concatenate(
            [on_j[k : k + 1] for k in range(weight.shape[2] // lanes)], axis=1
        )

    for copy in (to_core, core_east, core_north, core_far):
        copy.wait_recv()
    own.wait()

    def block_of(b):
        block = u1_all[:, g3[b]]
        block = block.reshape(cuts // 2, 2, tile, block.shape[2])
        one, two = block[:, 0], block[:, 1]
        one_t, two_t = pltpu.roll(one, half_tile, 1), pltpu.roll(two, half_tile, 1)
        re, im = jnp.where(upper, one, two_t), jnp.where(upper, one_t, two)
        both = jnp.concatenate((re, im), axis=0)
        return both.reshape(cuts * tile, both.shape[2])

    def in_two(x):
        hi = x.astype(jnp.bfloat16)
        return hi, (x - hi.astype(jnp.float32)).astype(jnp.bfloat16)

    mm = functools.partial(jnp.dot, preferred_element_type=jnp.float32)

    def apply_rows(p, carry):
        right = jnp.concatenate((block_of(p), block_of(p + pairs)), axis=0)
        rhi, rlo = in_two(right)
        left = base[p // 2, p % 2][None, None] * masks[...]
        lhi, llo = in_two(left.reshape(2 * cuts * tile, lanes))
        w = mm(lhi, rhi) + (mm(lhi, rlo) + mm(llo, rhi))
        w = w.reshape(2, cuts, tile, w.shape[1])
        for h in range(2):
            at = p + h * pairs
            wt[at] = jnp.sum(w[h] * weight[:, pl.ds(at, 1), :], axis=0)
        return carry

    lax.fori_loop(0, pairs, apply_rows, 0)

    for d in range(1, grps):
        sums[d].wait_recv()
        total = total + landed[d - 1]
    phis[...] = total.reshape(phis.shape)
    own_rows = phis.shape[1]
    place = pl.ds(c * own_rows, own_rows)
    phi[place] = phis[c]
    turned = []
    for d in range(1, cuts):
        to = (c + d) % cuts
        copy = pltpu.make_async_remote_copy(
            src_ref=phis.at[to], dst_ref=phi.at[place],
            send_sem=p_send.at[d - 1], recv_sem=p_recv.at[d - 1], device_id={"cuts": to},
        )
        copy.start()
        turned.append(copy)
    for copy in turned:
        copy.wait_recv()

    sign = jnp.where(lax.broadcasted_iota(jnp.int32, (tile, 1), 0) < half_tile, 1.0, -1.0)

    def fold(v):
        return functools.reduce(
            lambda p, q: p + q, [v[:, k : k + lanes] for k in range(0, v.shape[1], lanes)]
        )

    def one(b, carry):
        psi = phi[g0[b]]
        w = wt[b]
        swapped = pltpu.roll(psi, half_tile, 0)
        acc[0, pl.ds(b, 1), :] = jnp.sum(fold(w * psi) * sign, axis=0, keepdims=True)
        acc[1, pl.ds(b, 1), :] = jnp.sum(fold(w * swapped), axis=0, keepdims=True)
        return carry

    lax.fori_loop(0, count, one, 0, unroll=4)
    ones = jnp.ones((8, lanes), jnp.float32)
    add = lambda v: lax.dot_general(
        ones, v, (((1,), (1,)), ((), ())), precision=HI, preferred_element_type=jnp.float32
    )
    mine[...] = jnp.where(
        lax.broadcasted_iota(jnp.int32, mine.shape, 0) == 0, add(acc[0]), add(acc[1])
    )

    def everyone(axis, me, size, src, slots, send, recv):
        slots[me] = src[...]
        copies = []
        for d in range(1, size):
            to = (me + d) % size
            copy = pltpu.make_async_remote_copy(
                src_ref=src, dst_ref=slots.at[me],
                send_sem=send.at[d - 1], recv_sem=recv.at[d - 1], device_id={axis: to},
            )
            copy.start()
            copies.append(copy)
        for copy in copies:
            copy.wait()
        return functools.reduce(lambda p, q: p + q, [slots[k] for k in range(size)])

    mid[...] = everyone("grp", m, grps, mine, from_grp, g_send, g_recv)
    out[...] = everyone("cuts", c, cuts, mid, from_cuts, c_send, c_recv)
    for copy in (
        east_low, north_high, east_high, north_low, to_core, on_north, on_east,
        core_east, core_north, core_far, *row_copies, *sums.values(), *turned,
    ):
        copy.wait_send()


def make_fast_body(cuts, grps):

    def body(boundary, gate_stack, layer_order, cut_index, slice_bits, bitstrings):
        c = lax.axis_index("cuts")
        m = lax.axis_index("grp")
        n0, _, ext = boundary.shape[:3]
        pair = ext * ext
        rows = gate_stack.shape[2]
        kdim = n0 * ext
        cols = pair // grps
        width = ext // cuts
        own_rows = rows // ext
        g = group_digits(bitstrings)
        count = bitstrings.shape[0]
        f32 = jnp.float32

        gate0 = lax.dynamic_slice(gate_stack, (layer_order[0], 0, 0, m * kdim), (1, 2, rows, kdim))[0]
        big = jnp.stack((
            jnp.concatenate((gate0[0], -gate0[1]), axis=1),
            jnp.concatenate((gate0[1], gate0[0]), axis=1),
        ))
        big = big.reshape(2, own_rows, cuts, width, 2 * kdim)
        big = jnp.transpose(big, (2, 1, 0, 3, 4)).reshape(2 * rows, 2 * kdim)
        lh, ll = split(big)
        start = boundary.reshape(n0, 2, ext, pair)
        start = jnp.moveaxis(start, 1, 0).reshape(2 * kdim, pair)
        bh, bl = split(start)

        gate1 = lax.dynamic_slice(gate_stack, (layer_order[1], 0, 0, m * cols), (1, 2, rows, cols))[0]
        gate1 = jnp.transpose(gate1.reshape(2, own_rows, ext, cols), (2, 0, 1, 3))
        gate1 = gate1.reshape(ext, 2 * own_rows, cols)

        gate2 = lax.dynamic_index_in_dim(gate_stack, layer_order[2], 0, keepdims=False)
        wanted = g[1] * ext + g[2] - rows * c
        pick = (wanted[:, None] == jnp.arange(rows)[None, :]).astype(f32)
        picked = jnp.stack([jnp.dot(pick, gate2[k], precision=HI) for k in (0, 1)])
        picked = picked.reshape(2, 2, count // 2, cuts, width, ext)
        picked = jnp.transpose(picked, (3, 2, 4, 1, 0, 5)).reshape(cuts, count // 2 * width, 4 * ext)

        column = m * cols + jnp.arange(cols, dtype=jnp.int32)
        span = jnp.arange(ext, dtype=jnp.int32)
        tile, lanes = 2 * width, 4 * ext
        last = jnp.ones((1, count), f32)
        for group_id, layers in ((0, (0, 1, 2)), (1, (2,)), (2, (2,)), (3, (1, 2))):
            last = last * keep_mask(cut_index, slice_bits, layers, group_id, g[group_id])
        on_i1 = keep_mask(cut_index, slice_bits, (0, 1), 1, span)
        on_i2 = keep_mask(cut_index, slice_bits, (1,), 2, span)
        on_j = keep_mask(cut_index, slice_bits, (0,), 2, column // ext)
        on_j = on_j * keep_mask(cut_index, slice_bits, (0,), 3, column % ext)
        on_rows = jnp.tile(on_i1.reshape(cuts, width), (1, 2))
        on_rows = on_rows[:, :, None] * jnp.tile(on_i2, (1, 4))[None]
        on_b = jnp.pad(last, ((0, tile - 1), (0, lanes - count)))
        on_j = on_j.reshape(cols // lanes, lanes)
        on_j = jnp.pad(on_j, ((0, tile - on_j.shape[0]), (0, 0)))
        shared = jnp.broadcast_to(jnp.concatenate((on_b, on_j))[None], (cuts, 2 * tile, lanes))
        packed = jnp.concatenate((picked, on_rows, shared), axis=1)

        dma = pltpu.SemaphoreType.DMA
        smem = pl.BlockSpec(memory_space=pltpu.SMEM)
        small = (8, count)
        out = pl.pallas_call(
            functools.partial(whole_kernel, cuts, grps),
            out_shape=jax.ShapeDtypeStruct(small, f32),
            in_specs=[smem, smem] + [VMEM] * 6,
            out_specs=VMEM,
            scratch_shapes=[
                pltpu.VMEM((cuts,) + gate1.shape, f32),
                pltpu.VMEM((ext, tile, cols), f32),
                pltpu.VMEM((count // 4, 2, tile, lanes), f32),
                pltpu.VMEM((2, cuts, tile, lanes), f32),
                pltpu.VMEM((cuts, count, cols), f32),
                pltpu.VMEM((count, tile, cols), f32),
                pltpu.VMEM((grps - 1, 2 * rows, cols), f32),
                pltpu.VMEM((grps - 1, 2 * rows, cols), f32),
                pltpu.VMEM((cuts, own_rows, tile, cols), f32),
                pltpu.VMEM((cuts - 1,) + packed.shape[1:], f32),
                pltpu.VMEM((2, count, lanes), f32),
                pltpu.VMEM(small, f32), pltpu.VMEM((grps,) + small, f32),
                pltpu.VMEM(small, f32), pltpu.VMEM((cuts,) + small, f32),
                dma((10,)), dma((10,)), dma((grps - 1,)), dma((grps - 1,)),
                dma((cuts - 1,)), dma((cuts - 1,)), dma((cuts - 1,)), dma((cuts - 1,)), dma,
                dma((grps - 1,)), dma((grps - 1,)), dma((cuts - 1,)), dma((cuts - 1,)),
            ],
            compiler_params=pltpu.CompilerParams(
                collective_id=0, has_side_effects=True, vmem_limit_bytes=48 << 20
            ),
            name="whole",
        )(g[0], g[3], lh, ll, bh, bl, gate1, packed)
        return out[:2].T

    return body


def solution(mesh):
    fast = mesh.shape["cuts"] == 8
    maker = make_fast_body if fast else make_body
    return jax.shard_map(
        maker(mesh.shape["cuts"], mesh.shape["grp"]),
        mesh=mesh,
        in_specs=(
            P("grp", None, None, None, None),
            P(None, None, "cuts", None),
            P(),
            P(),
            P("cuts", None),
            P(),
        ),
        out_specs=P(),
        check_vma=False,
    )
```

```python
import functools

import jax
import jax.numpy as jnp
from jax import lax
from jax.experimental import pallas as pl
from jax.experimental.pallas import tpu as pltpu
from jax.sharding import PartitionSpec as P

LAYER_KINDS = (0, 1, 2, 3, 2, 3, 0, 1)
PAIR_GROUPS = ((0, 1), (2, 3), (1, 2), (1, 3))
PRECISION = lax.Precision.HIGH


def keep_mask(cut_index, slice_bits, layers, group_id, positions):
    hit = cut_index[:, 1] == group_id
    active = jnp.zeros_like(hit)
    for layer_id in layers:
        active = jnp.logical_or(active, cut_index[:, 0] == layer_id)
    active = jnp.logical_and(active, hit)
    bit_values = jnp.right_shift(positions[:, None], cut_index[None, :, 2]) & 1
    agrees = bit_values[None, :, :] == slice_bits[:, None, :]
    kept = jnp.logical_or(agrees, jnp.logical_not(active)[None, None, :])
    return jnp.all(kept, axis=2).astype(jnp.float32)


def group_digits(bitstrings):
    bits = bitstrings.shape[1] // 4
    weights = jnp.left_shift(jnp.ones((bits,), jnp.int32), jnp.arange(bits, dtype=jnp.int32))
    return [
        jnp.sum(bitstrings[:, k * bits : (k + 1) * bits] * weights, axis=1).astype(jnp.int32)
        for k in range(4)
    ]


def dot(a, b):
    return jnp.dot(a, b, precision=PRECISION, preferred_element_type=jnp.float32)


def make_body(cuts, grps):

    def body(boundary, gate_stack, layer_order, cut_index, slice_bits, bitstrings):
        c = lax.axis_index("cuts")
        m = lax.axis_index("grp")
        n0, _, ext = boundary.shape[:3]
        pair = ext * ext
        rows = gate_stack.shape[2]
        kdim = n0 * ext
        cols = pair // grps
        local_slices = slice_bits.shape[0]
        g = group_digits(bitstrings)
        count = bitstrings.shape[0]

        gate0 = lax.dynamic_index_in_dim(gate_stack, layer_order[0], 0, keepdims=False)
        gate0 = lax.dynamic_slice_in_dim(gate0, m * kdim, kdim, 2)
        start = jnp.moveaxis(boundary, 1, 0).reshape(2, kdim, pair)
        phi = jnp.stack((
            dot(gate0[0], start[0]) - dot(gate0[1], start[1]),
            dot(gate0[0], start[1]) + dot(gate0[1], start[0]),
        ))
        phi = lax.psum_scatter(phi, "grp", scatter_dimension=2, tiled=True)

        gate1 = lax.dynamic_index_in_dim(gate_stack, layer_order[1], 0, keepdims=False)
        gate1 = lax.dynamic_slice_in_dim(gate1, m * cols, cols, 2)
        gate1 = lax.all_gather(gate1, "cuts", axis=1, tiled=True)

        gate2 = lax.dynamic_index_in_dim(gate_stack, layer_order[2], 0, keepdims=False)
        wanted = g[1] * ext + g[2] - rows * c
        inside = jnp.logical_and(wanted >= 0, wanted < rows)
        picked = jnp.take(gate2, jnp.clip(wanted, 0, rows - 1), axis=1) * inside[None, :, None]
        if ext % cuts == 0:
            width, sub = ext // cuts, 1
            chunk = width * ext
            bits = jnp.zeros((2, cuts, local_slices, chunk), jnp.float32)
            bits = bits.at[:, :, :, : slice_bits.shape[1]].set(slice_bits.astype(jnp.float32))
            own = (jnp.arange(cuts) == c).astype(jnp.float32)
            bits = bits[:, :, None] * own[None, None, :, None, None]
            bits = bits.reshape(2, cuts, cuts * local_slices, chunk)
            bits = jnp.moveaxis(bits, 1, 2)
            packed = jnp.concatenate((picked.reshape(2, count, cuts, chunk), bits), axis=1)
            packed = lax.psum_scatter(packed, "cuts", scatter_dimension=2, tiled=True)[:, :, 0]
            gate2 = packed[:, :count].reshape(2, count, width, ext)
            slice_bits = packed[0, count:, : slice_bits.shape[1]].astype(jnp.int32)
            phi = phi.reshape(2, rows // ext, ext, cols)
            phi = lax.all_to_all(phi, "cuts", split_axis=2, concat_axis=1, tiled=True)
        else:
            width, sub = 1, cuts // ext
            slice_bits = lax.all_gather(slice_bits, "cuts", axis=0, tiled=True)
            picked = lax.psum(picked, "cuts").reshape(2, count, ext, ext)
            gate2 = lax.dynamic_slice_in_dim(picked, c // sub, 1, 2)
            phi = lax.all_gather(phi, "cuts", axis=1, tiled=True).reshape(2, ext, ext, cols)
            phi = lax.dynamic_slice_in_dim(phi, c // sub, 1, 2)
        first_i1 = c // sub * width
        cols = cols // sub
        first_col = (m * sub + c % sub) * cols
        if sub > 1:
            phi = lax.dynamic_slice_in_dim(phi, c % sub * cols, cols, 3)
            gate1 = lax.dynamic_slice_in_dim(gate1, c % sub * cols, cols, 2)

        slices = slice_bits.shape[0]
        column = first_col + jnp.arange(cols, dtype=jnp.int32)
        last = jnp.ones((slices, count), jnp.float32)
        for group_id, layers in ((0, (0, 1, 2)), (1, (2,)), (2, (2,)), (3, (1, 2))):
            last = last * keep_mask(cut_index, slice_bits, layers, group_id, g[group_id])
        on_i1 = keep_mask(
            cut_index, slice_bits, (0, 1), 1, first_i1 + jnp.arange(width, dtype=jnp.int32)
        )
        on_i2 = keep_mask(cut_index, slice_bits, (1,), 2, jnp.arange(ext, dtype=jnp.int32))
        on_j = keep_mask(cut_index, slice_bits, (0,), 2, column // ext)
        on_j = on_j * keep_mask(cut_index, slice_bits, (0,), 3, column % ext)

        left = gate2[:, :, None] * on_i2[None, None, :, None, :]
        left_re = jnp.concatenate((left[0], -left[1]), axis=3)
        left_im = jnp.concatenate((left[1], left[0]), axis=3)
        left = jnp.stack((left_re, left_im), axis=1)
        left = left.reshape(count, 2 * slices * width, 2 * ext)
        right = gate1.reshape(2, ext, ext, cols)
        right = jnp.take(jnp.moveaxis(right, 2, 0).reshape(ext, 2 * ext, cols), g[3], axis=0)
        w = lax.dot_general(
            left, right, (((2,), (1,)), ((0,), (0,))),
            precision=PRECISION, preferred_element_type=jnp.float32,
        )
        w = w.reshape(count, 2, slices, width, cols)
        scale = last.T[:, :, None, None] * on_i1[None, :, :, None] * on_j[None, :, None, :]
        w = jnp.sum(w * scale[:, None], axis=2)
        psi = jnp.take(phi, g[0], axis=1)
        real = jnp.sum(w[:, 0] * psi[0] - w[:, 1] * psi[1], axis=(1, 2))
        imag = jnp.sum(w[:, 0] * psi[1] + w[:, 1] * psi[0], axis=(1, 2))
        return lax.psum(jnp.stack((real, imag), axis=1), ("cuts", "grp"))

    return body


VMEM = pl.BlockSpec(memory_space=pltpu.VMEM)
HI = lax.Precision.HIGHEST


def split(x):
    hi = lax.reduce_precision(x, 8, 7)
    return hi.astype(jnp.bfloat16), (x - hi).astype(jnp.bfloat16)


def flip(index, step):
    return index + step * (1 - 2 * ((index // step) % 2))


def greet(cuts, grps):
    c, m = lax.axis_index("cuts"), lax.axis_index("grp")
    barrier = pltpu.get_barrier_semaphore()
    for d in range(1, cuts):
        pl.semaphore_signal(barrier, inc=1, device_id={"cuts": (c + d) % cuts})
    for d in range(1, grps):
        pl.semaphore_signal(barrier, inc=1, device_id={"grp": (m + d) % grps})
    pl.semaphore_wait(barrier, cuts + grps - 2)
    return c, m


def whole_kernel(
    cuts, grps, g0, g3, lh, ll, bh, bl, u1, packed, out,
    u1_all, phi, base, masks, weight, wt,
    parts, landed, phis, u2_in, acc, mine, from_grp, mid, from_cuts,
    u_send, u_recv, r_send, r_recv, p_send, p_recv, k_send, k_recv, own_sem,
    g_send, g_recv, c_send, c_recv,
):
    c, m = greet(cuts, grps)
    core, east, north = flip(c, 1), flip(c, 2), flip(c, 4)
    half = u1.shape[0] // 2
    low, high = pl.ds(0, half), pl.ds(half, half)

    def send_u1(slot, src, dst, target):
        return pltpu.make_async_remote_copy(
            src_ref=src, dst_ref=dst, send_sem=u_send.at[slot], recv_sem=u_recv.at[slot],
            device_id={"cuts": target},
        )

    own = pltpu.make_async_copy(u1, u1_all.at[c], own_sem)
    own.start()
    east_low = send_u1(0, u1.at[low], u1_all.at[c, low], east)
    north_high = send_u1(1, u1.at[high], u1_all.at[c, high], north)
    east_high = send_u1(2, u1.at[high], u1_all.at[c, high], east)
    north_low = send_u1(3, u1.at[low], u1_all.at[c, low], north)
    to_core = send_u1(4, u1, u1_all.at[c], core)
    for copy in (east_low, north_high, east_high, north_low, to_core):
        copy.start()

    row_copies = []
    for d in range(1, cuts):
        to = (c + d) % cuts
        copy = pltpu.make_async_remote_copy(
            src_ref=packed.at[to], dst_ref=u2_in.at[d - 1],
            send_sem=k_send.at[d - 1], recv_sem=k_recv.at[d - 1], device_id={"cuts": to},
        )
        row_copies.append(copy)

    cols = parts.shape[2]

    def product(part):
        at = pl.ds(pl.multiple_of(part * cols, cols), cols)
        bhi, blo = bh[:, at], bl[:, at]
        mm = functools.partial(jnp.dot, preferred_element_type=jnp.float32)
        return mm(lh[...], bhi) + (mm(lh[...], blo) + mm(ll[...], bhi))

    sums = {}
    for d in sorted(range(1, grps), key=lambda d: -min(d, grps - d)):
        to = (m + d) % grps
        parts[d - 1] = product(to)
        sums[d] = pltpu.make_async_remote_copy(
            src_ref=parts.at[d - 1], dst_ref=landed.at[d - 1],
            send_sem=r_send.at[d - 1], recv_sem=r_recv.at[d - 1], device_id={"grp": to},
        )
        sums[d].start()
    total = product(m)

    east_low.wait_recv()
    on_north = send_u1(5, u1_all.at[east, low], u1_all.at[east, low], north)
    on_north.start()
    north_high.wait_recv()
    on_east = send_u1(6, u1_all.at[north, high], u1_all.at[north, high], east)
    on_east.start()
    for copy in row_copies:
        copy.start()
    east_high.wait_recv()
    core_east = send_u1(7, u1_all.at[east], u1_all.at[east], core)
    core_east.start()
    north_low.wait_recv()
    core_north = send_u1(8, u1_all.at[north], u1_all.at[north], core)
    core_north.start()
    on_north.wait_recv()
    on_east.wait_recv()
    far = flip(east, 4)
    core_far = send_u1(9, u1_all.at[far], u1_all.at[far], core)
    core_far.start()


    lanes = packed.shape[2]
    tile = phi.shape[1]
    half_tile = tile // 2
    count = wt.shape[0]
    pairs = count // 2
    picked_rows = pairs * half_tile
    for d in range(1, cuts):
        row_copies[d - 1].wait_recv()
    rows = packed[c, pl.ds(0, picked_rows)]
    for d in range(1, cuts):
        rows = rows + u2_in[d - 1, pl.ds(0, picked_rows)]
    rows = rows.reshape(picked_rows // tile, tile, lanes)
    lane = lax.broadcasted_iota(jnp.int32, (1, 1, lanes), 2)
    row = lax.broadcasted_iota(jnp.int32, (1, tile, 1), 1)
    quarter = lanes // 4
    even = (lane // quarter) % 2 == 0
    real_rows = jnp.where(even, rows, -rows)
    imag_rows = jnp.where(even, pltpu.roll(rows, lanes - quarter, 2), pltpu.roll(rows, quarter, 2))
    upper = row < half_tile
    base[:, 0] = jnp.where(upper, real_rows, pltpu.roll(imag_rows, half_tile, 1))
    base[:, 1] = jnp.where(upper, pltpu.roll(real_rows, half_tile, 1), imag_rows)
    first = lax.broadcasted_iota(jnp.int32, (1, lanes), 1) < lanes // 2
    for s in range(cuts):
        slot = packed.at[c] if s == 0 else u2_in.at[s - 1]
        mask = slot[pl.ds(picked_rows, tile)]
        masks[0, s] = jnp.where(first, mask, 0.0)
        masks[1, s] = jnp.where(first, 0.0, mask)
        on_b = slot[pl.ds(picked_rows + tile, tile)]
        on_j = slot[pl.ds(picked_rows + 2 * tile, tile)]
        column = jnp.transpose(on_b)[:count, 0:1]
        weight[s] = column * jnp.concatenate(
            [on_j[k : k + 1] for k in range(weight.shape[2] // lanes)], axis=1
        )

    for copy in (to_core, core_east, core_north, core_far):
        copy.wait_recv()
    own.wait()

    def block_of(b):
        block = u1_all[:, g3[b]]
        block = block.reshape(cuts // 2, 2, tile, block.shape[2])
        one, two = block[:, 0], block[:, 1]
        one_t, two_t = pltpu.roll(one, half_tile, 1), pltpu.roll(two, half_tile, 1)
        re, im = jnp.where(upper, one, two_t), jnp.where(upper, one_t, two)
        both = jnp.concatenate((re, im), axis=0)
        return both.reshape(cuts * tile, both.shape[2])

    def in_two(x):
        hi = x.astype(jnp.bfloat16)
        return hi, (x - hi.astype(jnp.float32)).astype(jnp.bfloat16)

    mm = functools.partial(jnp.dot, preferred_element_type=jnp.float32)

    def apply_rows(p, carry):
        right = jnp.concatenate((block_of(p), block_of(p + pairs)), axis=0)
        rhi, rlo = in_two(right)
        left = base[p // 2, p % 2][None, None] * masks[...]
        lhi, llo = in_two(left.reshape(2 * cuts * tile, lanes))
        w = mm(lhi, rhi) + (mm(lhi, rlo) + mm(llo, rhi))
        w = w.reshape(2, cuts, tile, w.shape[1])
        for h in range(2):
            at = p + h * pairs
            wt[at] = jnp.sum(w[h] * weight[:, pl.ds(at, 1), :], axis=0)
        return carry

    lax.fori_loop(0, pairs, apply_rows, 0)

    for d in range(1, grps):
        sums[d].wait_recv()
        total = total + landed[d - 1]
    phis[...] = total.reshape(phis.shape)
    own_rows = phis.shape[1]
    place = pl.ds(c * own_rows, own_rows)
    phi[place] = phis[c]
    turned = []
    for d in range(1, cuts):
        to = (c + d) % cuts
        copy = pltpu.make_async_remote_copy(
            src_ref=phis.at[to], dst_ref=phi.at[place],
            send_sem=p_send.at[d - 1], recv_sem=p_recv.at[d - 1], device_id={"cuts": to},
        )
        copy.start()
        turned.append(copy)
    for copy in turned:
        copy.wait_recv()

    sign = jnp.where(lax.broadcasted_iota(jnp.int32, (tile, 1), 0) < half_tile, 1.0, -1.0)

    def fold(v):
        return functools.reduce(
            lambda p, q: p + q, [v[:, k : k + lanes] for k in range(0, v.shape[1], lanes)]
        )

    def one(b, carry):
        psi = phi[g0[b]]
        w = wt[b]
        swapped = pltpu.roll(psi, half_tile, 0)
        acc[0, pl.ds(b, 1), :] = jnp.sum(fold(w * psi) * sign, axis=0, keepdims=True)
        acc[1, pl.ds(b, 1), :] = jnp.sum(fold(w * swapped), axis=0, keepdims=True)
        return carry

    lax.fori_loop(0, count, one, 0, unroll=4)
    ones = jnp.ones((8, lanes), jnp.float32)
    add = lambda v: lax.dot_general(
        ones, v, (((1,), (1,)), ((), ())), precision=HI, preferred_element_type=jnp.float32
    )
    mine[...] = jnp.where(
        lax.broadcasted_iota(jnp.int32, mine.shape, 0) == 0, add(acc[0]), add(acc[1])
    )

    def everyone(axis, me, size, src, slots, send, recv):
        slots[me] = src[...]
        copies = []
        for d in range(1, size):
            to = (me + d) % size
            copy = pltpu.make_async_remote_copy(
                src_ref=src, dst_ref=slots.at[me],
                send_sem=send.at[d - 1], recv_sem=recv.at[d - 1], device_id={axis: to},
            )
            copy.start()
            copies.append(copy)
        for copy in copies:
            copy.wait()
        return functools.reduce(lambda p, q: p + q, [slots[k] for k in range(size)])

    mid[...] = everyone("grp", m, grps, mine, from_grp, g_send, g_recv)
    out[...] = everyone("cuts", c, cuts, mid, from_cuts, c_send, c_recv)
    for copy in (
        east_low, north_high, east_high, north_low, to_core, on_north, on_east,
        core_east, core_north, core_far, *row_copies, *sums.values(), *turned,
    ):
        copy.wait_send()


def make_fast_body(cuts, grps):

    def body(boundary, gate_stack, layer_order, cut_index, slice_bits, bitstrings):
        c = lax.axis_index("cuts")
        m = lax.axis_index("grp")
        n0, _, ext = boundary.shape[:3]
        pair = ext * ext
        rows = gate_stack.shape[2]
        kdim = n0 * ext
        cols = pair // grps
        width = ext // cuts
        own_rows = rows // ext
        g = group_digits(bitstrings)
        count = bitstrings.shape[0]
        f32 = jnp.float32
        u32 = jnp.uint32
        order = layer_order.astype(u32)
        zero = u32(0)
        spot = m.astype(u32)

        gate0 = lax.dynamic_slice(gate_stack, (order[0], zero, zero, spot * u32(kdim)), (1, 2, rows, kdim))[0]
        big = jnp.stack((
            jnp.concatenate((gate0[0], -gate0[1]), axis=1),
            jnp.concatenate((gate0[1], gate0[0]), axis=1),
        ))
        big = big.reshape(2, own_rows, cuts, width, 2 * kdim)
        big = jnp.transpose(big, (2, 1, 0, 3, 4)).reshape(2 * rows, 2 * kdim)
        lh, ll = split(big)
        start = boundary.reshape(n0, 2, ext, pair)
        start = jnp.moveaxis(start, 1, 0).reshape(2 * kdim, pair)
        bh, bl = split(start)

        gate1 = lax.dynamic_slice(gate_stack, (order[1], zero, zero, spot * u32(cols)), (1, 2, rows, cols))[0]
        gate1 = jnp.transpose(gate1.reshape(2, own_rows, ext, cols), (2, 0, 1, 3))
        gate1 = gate1.reshape(ext, 2 * own_rows, cols)

        gate2 = lax.dynamic_slice(gate_stack, (order[2], zero, zero, zero), (1,) + gate_stack.shape[1:])[0]
        wanted = g[1] * ext + g[2] - rows * c
        pick = (wanted[:, None] == jnp.arange(rows)[None, :]).astype(f32)
        picked = lax.dot_general(pick, gate2, (((1,), (1,)), ((), ())), precision=HI)
        picked = picked.reshape(2, count // 2, 2, cuts, width, ext)
        picked = jnp.transpose(picked, (3, 1, 4, 0, 2, 5)).reshape(cuts, count // 2 * width, 4 * ext)

        column = m * cols + jnp.arange(cols, dtype=jnp.int32)
        span = jnp.arange(ext, dtype=jnp.int32)
        tile, lanes = 2 * width, 4 * ext
        wants = (
            (0, 7, g[0]), (1, 4, g[1]), (2, 4, g[2]), (3, 6, g[3]), (1, 3, span), (2, 2, span),
            (2, 1, column // ext), (3, 1, column % ext),
        )
        places = jnp.concatenate([place for _, _, place in wants])
        group_of = jnp.concatenate([jnp.full(p.shape, k, jnp.int32) for k, _, p in wants])
        layers_of = jnp.concatenate([jnp.full(p.shape, bits, jnp.int32) for _, bits, p in wants])
        layer, group, bit = (cut_index[:, k : k + 1] for k in range(3))
        active = (group == group_of[None]) & ((jnp.right_shift(layers_of[None], layer) & 1) == 1)
        agrees = (jnp.right_shift(places[None], bit) & 1) == slice_bits.reshape(-1, 1)
        kept = jnp.min(jnp.where(active & ~agrees, 0.0, 1.0), axis=0)
        pieces, at = [], 0
        for _, _, place in wants:
            pieces.append(kept[at : at + place.shape[0]][None])
            at += place.shape[0]
        last = pieces[0] * pieces[1] * pieces[2] * pieces[3]
        on_i1, on_i2 = pieces[4], pieces[5]
        on_j = pieces[6] * pieces[7]
        on_rows = jnp.tile(on_i1.reshape(cuts, width), (1, 2))
        on_rows = on_rows[:, :, None] * jnp.tile(on_i2, (1, 4))[None]
        on_b = jnp.pad(last, ((0, tile - 1), (0, lanes - count)))
        on_j = on_j.reshape(cols // lanes, lanes)
        on_j = jnp.pad(on_j, ((0, tile - on_j.shape[0]), (0, 0)))
        shared = jnp.broadcast_to(jnp.concatenate((on_b, on_j))[None], (cuts, 2 * tile, lanes))
        packed = jnp.concatenate((picked, on_rows, shared), axis=1)

        dma = pltpu.SemaphoreType.DMA
        smem = pl.BlockSpec(memory_space=pltpu.SMEM)
        small = (8, count)
        out = pl.pallas_call(
            functools.partial(whole_kernel, cuts, grps),
            out_shape=jax.ShapeDtypeStruct(small, f32),
            in_specs=[smem, smem] + [VMEM] * 6,
            out_specs=VMEM,
            scratch_shapes=[
                pltpu.VMEM((cuts,) + gate1.shape, f32),
                pltpu.VMEM((ext, tile, cols), f32),
                pltpu.VMEM((count // 4, 2, tile, lanes), f32),
                pltpu.VMEM((2, cuts, tile, lanes), f32),
                pltpu.VMEM((cuts, count, cols), f32),
                pltpu.VMEM((count, tile, cols), f32),
                pltpu.VMEM((grps - 1, 2 * rows, cols), f32),
                pltpu.VMEM((grps - 1, 2 * rows, cols), f32),
                pltpu.VMEM((cuts, own_rows, tile, cols), f32),
                pltpu.VMEM((cuts - 1,) + packed.shape[1:], f32),
                pltpu.VMEM((2, count, lanes), f32),
                pltpu.VMEM(small, f32), pltpu.VMEM((grps,) + small, f32),
                pltpu.VMEM(small, f32), pltpu.VMEM((cuts,) + small, f32),
                dma((10,)), dma((10,)), dma((grps - 1,)), dma((grps - 1,)),
                dma((cuts - 1,)), dma((cuts - 1,)), dma((cuts - 1,)), dma((cuts - 1,)), dma,
                dma((grps - 1,)), dma((grps - 1,)), dma((cuts - 1,)), dma((cuts - 1,)),
            ],
            compiler_params=pltpu.CompilerParams(
                collective_id=0, has_side_effects=True, vmem_limit_bytes=48 << 20
            ),
            name="whole",
        )(g[0], g[3], lh, ll, bh, bl, gate1, packed)
        return out[:2].T

    return body


def solution(mesh):
    fast = mesh.shape["cuts"] == 8
    maker = make_fast_body if fast else make_body
    return jax.shard_map(
        maker(mesh.shape["cuts"], mesh.shape["grp"]),
        mesh=mesh,
        in_specs=(
            P("grp", None, None, None, None),
            P(None, None, "cuts", None),
            P(),
            P(),
            P("cuts", None),
            P(),
        ),
        out_specs=P(),
        check_vma=False,
    )
```

```python
import functools

import jax
import jax.numpy as jnp
from jax import lax
from jax.experimental import pallas as pl
from jax.experimental.pallas import tpu as pltpu
from jax.sharding import PartitionSpec as P

LAYER_KINDS = (0, 1, 2, 3, 2, 3, 0, 1)
PAIR_GROUPS = ((0, 1), (2, 3), (1, 2), (1, 3))
PRECISION = lax.Precision.HIGH


def keep_mask(cut_index, slice_bits, layers, group_id, positions):
    hit = cut_index[:, 1] == group_id
    active = jnp.zeros_like(hit)
    for layer_id in layers:
        active = jnp.logical_or(active, cut_index[:, 0] == layer_id)
    active = jnp.logical_and(active, hit)
    bit_values = jnp.right_shift(positions[:, None], cut_index[None, :, 2]) & 1
    agrees = bit_values[None, :, :] == slice_bits[:, None, :]
    kept = jnp.logical_or(agrees, jnp.logical_not(active)[None, None, :])
    return jnp.all(kept, axis=2).astype(jnp.float32)


def group_digits(bitstrings):
    bits = bitstrings.shape[1] // 4
    weights = jnp.left_shift(jnp.ones((bits,), jnp.int32), jnp.arange(bits, dtype=jnp.int32))
    return [
        jnp.sum(bitstrings[:, k * bits : (k + 1) * bits] * weights, axis=1).astype(jnp.int32)
        for k in range(4)
    ]


def dot(a, b):
    return jnp.dot(a, b, precision=PRECISION, preferred_element_type=jnp.float32)


def make_body(cuts, grps):

    def body(boundary, gate_stack, layer_order, cut_index, slice_bits, bitstrings):
        c = lax.axis_index("cuts")
        m = lax.axis_index("grp")
        n0, _, ext = boundary.shape[:3]
        pair = ext * ext
        rows = gate_stack.shape[2]
        kdim = n0 * ext
        cols = pair // grps
        local_slices = slice_bits.shape[0]
        g = group_digits(bitstrings)
        count = bitstrings.shape[0]

        gate0 = lax.dynamic_index_in_dim(gate_stack, layer_order[0], 0, keepdims=False)
        gate0 = lax.dynamic_slice_in_dim(gate0, m * kdim, kdim, 2)
        start = jnp.moveaxis(boundary, 1, 0).reshape(2, kdim, pair)
        phi = jnp.stack((
            dot(gate0[0], start[0]) - dot(gate0[1], start[1]),
            dot(gate0[0], start[1]) + dot(gate0[1], start[0]),
        ))
        phi = lax.psum_scatter(phi, "grp", scatter_dimension=2, tiled=True)

        gate1 = lax.dynamic_index_in_dim(gate_stack, layer_order[1], 0, keepdims=False)
        gate1 = lax.dynamic_slice_in_dim(gate1, m * cols, cols, 2)
        gate1 = lax.all_gather(gate1, "cuts", axis=1, tiled=True)

        gate2 = lax.dynamic_index_in_dim(gate_stack, layer_order[2], 0, keepdims=False)
        wanted = g[1] * ext + g[2] - rows * c
        inside = jnp.logical_and(wanted >= 0, wanted < rows)
        picked = jnp.take(gate2, jnp.clip(wanted, 0, rows - 1), axis=1) * inside[None, :, None]
        if ext % cuts == 0:
            width, sub = ext // cuts, 1
            chunk = width * ext
            bits = jnp.zeros((2, cuts, local_slices, chunk), jnp.float32)
            bits = bits.at[:, :, :, : slice_bits.shape[1]].set(slice_bits.astype(jnp.float32))
            own = (jnp.arange(cuts) == c).astype(jnp.float32)
            bits = bits[:, :, None] * own[None, None, :, None, None]
            bits = bits.reshape(2, cuts, cuts * local_slices, chunk)
            bits = jnp.moveaxis(bits, 1, 2)
            packed = jnp.concatenate((picked.reshape(2, count, cuts, chunk), bits), axis=1)
            packed = lax.psum_scatter(packed, "cuts", scatter_dimension=2, tiled=True)[:, :, 0]
            gate2 = packed[:, :count].reshape(2, count, width, ext)
            slice_bits = packed[0, count:, : slice_bits.shape[1]].astype(jnp.int32)
            phi = phi.reshape(2, rows // ext, ext, cols)
            phi = lax.all_to_all(phi, "cuts", split_axis=2, concat_axis=1, tiled=True)
        else:
            width, sub = 1, cuts // ext
            slice_bits = lax.all_gather(slice_bits, "cuts", axis=0, tiled=True)
            picked = lax.psum(picked, "cuts").reshape(2, count, ext, ext)
            gate2 = lax.dynamic_slice_in_dim(picked, c // sub, 1, 2)
            phi = lax.all_gather(phi, "cuts", axis=1, tiled=True).reshape(2, ext, ext, cols)
            phi = lax.dynamic_slice_in_dim(phi, c // sub, 1, 2)
        first_i1 = c // sub * width
        cols = cols // sub
        first_col = (m * sub + c % sub) * cols
        if sub > 1:
            phi = lax.dynamic_slice_in_dim(phi, c % sub * cols, cols, 3)
            gate1 = lax.dynamic_slice_in_dim(gate1, c % sub * cols, cols, 2)

        slices = slice_bits.shape[0]
        column = first_col + jnp.arange(cols, dtype=jnp.int32)
        last = jnp.ones((slices, count), jnp.float32)
        for group_id, layers in ((0, (0, 1, 2)), (1, (2,)), (2, (2,)), (3, (1, 2))):
            last = last * keep_mask(cut_index, slice_bits, layers, group_id, g[group_id])
        on_i1 = keep_mask(
            cut_index, slice_bits, (0, 1), 1, first_i1 + jnp.arange(width, dtype=jnp.int32)
        )
        on_i2 = keep_mask(cut_index, slice_bits, (1,), 2, jnp.arange(ext, dtype=jnp.int32))
        on_j = keep_mask(cut_index, slice_bits, (0,), 2, column // ext)
        on_j = on_j * keep_mask(cut_index, slice_bits, (0,), 3, column % ext)

        left = gate2[:, :, None] * on_i2[None, None, :, None, :]
        left_re = jnp.concatenate((left[0], -left[1]), axis=3)
        left_im = jnp.concatenate((left[1], left[0]), axis=3)
        left = jnp.stack((left_re, left_im), axis=1)
        left = left.reshape(count, 2 * slices * width, 2 * ext)
        right = gate1.reshape(2, ext, ext, cols)
        right = jnp.take(jnp.moveaxis(right, 2, 0).reshape(ext, 2 * ext, cols), g[3], axis=0)
        w = lax.dot_general(
            left, right, (((2,), (1,)), ((0,), (0,))),
            precision=PRECISION, preferred_element_type=jnp.float32,
        )
        w = w.reshape(count, 2, slices, width, cols)
        scale = last.T[:, :, None, None] * on_i1[None, :, :, None] * on_j[None, :, None, :]
        w = jnp.sum(w * scale[:, None], axis=2)
        psi = jnp.take(phi, g[0], axis=1)
        real = jnp.sum(w[:, 0] * psi[0] - w[:, 1] * psi[1], axis=(1, 2))
        imag = jnp.sum(w[:, 0] * psi[1] + w[:, 1] * psi[0], axis=(1, 2))
        return lax.psum(jnp.stack((real, imag), axis=1), ("cuts", "grp"))

    return body


VMEM = pl.BlockSpec(memory_space=pltpu.VMEM)
HI = lax.Precision.HIGHEST


def split(x):
    hi = lax.reduce_precision(x, 8, 7)
    return hi.astype(jnp.bfloat16), (x - hi).astype(jnp.bfloat16)


def flip(index, step):
    return index + step * (1 - 2 * ((index // step) % 2))


def greet(cuts, grps):
    c, m = lax.axis_index("cuts"), lax.axis_index("grp")
    barrier = pltpu.get_barrier_semaphore()
    for d in range(1, cuts):
        pl.semaphore_signal(barrier, inc=1, device_id={"cuts": (c + d) % cuts})
    for d in range(1, grps):
        pl.semaphore_signal(barrier, inc=1, device_id={"grp": (m + d) % grps})
    pl.semaphore_wait(barrier, cuts + grps - 2)
    return c, m


def whole_kernel(
    cuts, grps, g0, g3, lh, ll, bh, bl, u1, packed, out,
    u1_all, phi, base, masks, weight, wt,
    parts, landed, phis, u2_in, acc, mine, from_grp, mid, from_cuts,
    u_send, u_recv, r_send, r_recv, p_send, p_recv, k_send, k_recv, own_sem,
    g_send, g_recv, c_send, c_recv,
):
    c, m = greet(cuts, grps)
    core, east, north = flip(c, 1), flip(c, 2), flip(c, 4)
    half = u1.shape[0] // 2
    low, high = pl.ds(0, half), pl.ds(half, half)

    def send_u1(slot, src, dst, target):
        return pltpu.make_async_remote_copy(
            src_ref=src, dst_ref=dst, send_sem=u_send.at[slot], recv_sem=u_recv.at[slot],
            device_id={"cuts": target},
        )

    own = pltpu.make_async_copy(u1, u1_all.at[c], own_sem)
    own.start()
    east_low = send_u1(0, u1.at[low], u1_all.at[c, low], east)
    north_high = send_u1(1, u1.at[high], u1_all.at[c, high], north)
    east_high = send_u1(2, u1.at[high], u1_all.at[c, high], east)
    north_low = send_u1(3, u1.at[low], u1_all.at[c, low], north)
    to_core = send_u1(4, u1, u1_all.at[c], core)
    for copy in (east_low, north_high, east_high, north_low, to_core):
        copy.start()

    row_copies = []
    for d in range(1, cuts):
        to = (c + d) % cuts
        copy = pltpu.make_async_remote_copy(
            src_ref=packed.at[to], dst_ref=u2_in.at[d - 1],
            send_sem=k_send.at[d - 1], recv_sem=k_recv.at[d - 1], device_id={"cuts": to},
        )
        row_copies.append(copy)

    cols = parts.shape[2]

    def product(part):
        at = pl.ds(pl.multiple_of(part * cols, cols), cols)
        bhi, blo = bh[:, at], bl[:, at]
        mm = functools.partial(jnp.dot, preferred_element_type=jnp.float32)
        return mm(lh[...], bhi) + (mm(lh[...], blo) + mm(ll[...], bhi))

    near, across = flip(m, 1), flip(m, 2)

    def send_sum(slot, target):
        return pltpu.make_async_remote_copy(
            src_ref=parts.at[slot], dst_ref=landed.at[slot],
            send_sem=r_send.at[slot], recv_sem=r_recv.at[slot], device_id={"grp": target},
        )

    sums = [send_sum(0, near), send_sum(1, near), send_sum(2, across)]
    parts[0] = product(flip(near, 2))
    sums[0].start()
    parts[1] = product(near)
    sums[1].start()
    carried = product(across)
    total = product(m)

    east_low.wait_recv()
    on_north = send_u1(5, u1_all.at[east, low], u1_all.at[east, low], north)
    on_north.start()
    north_high.wait_recv()
    on_east = send_u1(6, u1_all.at[north, high], u1_all.at[north, high], east)
    on_east.start()
    for copy in row_copies:
        copy.start()
    sums[0].wait_recv()
    parts[2] = carried + landed[0]
    sums[2].start()
    east_high.wait_recv()
    core_east = send_u1(7, u1_all.at[east], u1_all.at[east], core)
    core_east.start()
    north_low.wait_recv()
    core_north = send_u1(8, u1_all.at[north], u1_all.at[north], core)
    core_north.start()
    on_north.wait_recv()
    on_east.wait_recv()
    far = flip(east, 4)
    core_far = send_u1(9, u1_all.at[far], u1_all.at[far], core)
    core_far.start()


    lanes = packed.shape[2]
    tile = phi.shape[1]
    half_tile = tile // 2
    count = wt.shape[0]
    pairs = count // 2
    picked_rows = pairs * half_tile
    for d in range(1, cuts):
        row_copies[d - 1].wait_recv()
    rows = packed[c, pl.ds(0, picked_rows)]
    for d in range(1, cuts):
        rows = rows + u2_in[d - 1, pl.ds(0, picked_rows)]
    rows = rows.reshape(picked_rows // tile, tile, lanes)
    lane = lax.broadcasted_iota(jnp.int32, (1, 1, lanes), 2)
    row = lax.broadcasted_iota(jnp.int32, (1, tile, 1), 1)
    quarter = lanes // 4
    even = (lane // quarter) % 2 == 0
    real_rows = jnp.where(even, rows, -rows)
    imag_rows = jnp.where(even, pltpu.roll(rows, lanes - quarter, 2), pltpu.roll(rows, quarter, 2))
    upper = row < half_tile
    base[:, 0] = jnp.where(upper, real_rows, pltpu.roll(imag_rows, half_tile, 1))
    base[:, 1] = jnp.where(upper, pltpu.roll(real_rows, half_tile, 1), imag_rows)
    first = lax.broadcasted_iota(jnp.int32, (1, lanes), 1) < lanes // 2
    for s in range(cuts):
        slot = packed.at[c] if s == 0 else u2_in.at[s - 1]
        mask = slot[pl.ds(picked_rows, tile)]
        masks[0, s] = jnp.where(first, mask, 0.0)
        masks[1, s] = jnp.where(first, 0.0, mask)
        on_b = slot[pl.ds(picked_rows + tile, tile)]
        on_j = slot[pl.ds(picked_rows + 2 * tile, tile)]
        column = jnp.transpose(on_b)[:count, 0:1]
        weight[s] = column * jnp.concatenate(
            [on_j[k : k + 1] for k in range(weight.shape[2] // lanes)], axis=1
        )

    for copy in (to_core, core_east, core_north, core_far):
        copy.wait_recv()
    own.wait()

    def block_of(b):
        block = u1_all[:, g3[b]]
        block = block.reshape(cuts // 2, 2, tile, block.shape[2])
        one, two = block[:, 0], block[:, 1]
        one_t, two_t = pltpu.roll(one, half_tile, 1), pltpu.roll(two, half_tile, 1)
        re, im = jnp.where(upper, one, two_t), jnp.where(upper, one_t, two)
        both = jnp.concatenate((re, im), axis=0)
        return both.reshape(cuts * tile, both.shape[2])

    def in_two(x):
        hi = x.astype(jnp.bfloat16)
        return hi, (x - hi.astype(jnp.float32)).astype(jnp.bfloat16)

    mm = functools.partial(jnp.dot, preferred_element_type=jnp.float32)

    def apply_rows(p, carry):
        right = jnp.concatenate((block_of(p), block_of(p + pairs)), axis=0)
        rhi, rlo = in_two(right)
        left = base[p // 2, p % 2][None, None] * masks[...]
        lhi, llo = in_two(left.reshape(2 * cuts * tile, lanes))
        w = mm(lhi, rhi) + (mm(lhi, rlo) + mm(llo, rhi))
        w = w.reshape(2, cuts, tile, w.shape[1])
        for h in range(2):
            at = p + h * pairs
            wt[at] = jnp.sum(w[h] * weight[:, pl.ds(at, 1), :], axis=0)
        return carry

    lax.fori_loop(0, pairs, apply_rows, 0)

    for slot in (1, 2):
        sums[slot].wait_recv()
        total = total + landed[slot]
    phis[...] = total.reshape(phis.shape)
    own_rows = phis.shape[1]
    place = pl.ds(c * own_rows, own_rows)
    phi[place] = phis[c]
    turned = []
    for d in range(1, cuts):
        to = (c + d) % cuts
        copy = pltpu.make_async_remote_copy(
            src_ref=phis.at[to], dst_ref=phi.at[place],
            send_sem=p_send.at[d - 1], recv_sem=p_recv.at[d - 1], device_id={"cuts": to},
        )
        copy.start()
        turned.append(copy)
    for copy in turned:
        copy.wait_recv()

    sign = jnp.where(lax.broadcasted_iota(jnp.int32, (tile, 1), 0) < half_tile, 1.0, -1.0)

    def fold(v):
        return functools.reduce(
            lambda p, q: p + q, [v[:, k : k + lanes] for k in range(0, v.shape[1], lanes)]
        )

    def one(b, carry):
        psi = phi[g0[b]]
        w = wt[b]
        swapped = pltpu.roll(psi, half_tile, 0)
        acc[0, pl.ds(b, 1), :] = jnp.sum(fold(w * psi) * sign, axis=0, keepdims=True)
        acc[1, pl.ds(b, 1), :] = jnp.sum(fold(w * swapped), axis=0, keepdims=True)
        return carry

    lax.fori_loop(0, count, one, 0, unroll=4)
    ones = jnp.ones((8, lanes), jnp.float32)
    add = lambda v: lax.dot_general(
        ones, v, (((1,), (1,)), ((), ())), precision=HI, preferred_element_type=jnp.float32
    )
    mine[...] = jnp.where(
        lax.broadcasted_iota(jnp.int32, mine.shape, 0) == 0, add(acc[0]), add(acc[1])
    )

    def everyone(axis, me, size, src, slots, send, recv):
        slots[me] = src[...]
        copies = []
        for d in range(1, size):
            to = (me + d) % size
            copy = pltpu.make_async_remote_copy(
                src_ref=src, dst_ref=slots.at[me],
                send_sem=send.at[d - 1], recv_sem=recv.at[d - 1], device_id={axis: to},
            )
            copy.start()
            copies.append(copy)
        for copy in copies:
            copy.wait()
        return functools.reduce(lambda p, q: p + q, [slots[k] for k in range(size)])

    mid[...] = everyone("grp", m, grps, mine, from_grp, g_send, g_recv)
    out[...] = everyone("cuts", c, cuts, mid, from_cuts, c_send, c_recv)
    for copy in (
        east_low, north_high, east_high, north_low, to_core, on_north, on_east,
        core_east, core_north, core_far, *row_copies, *sums, *turned,
    ):
        copy.wait_send()


def make_fast_body(cuts, grps):

    def body(boundary, gate_stack, layer_order, cut_index, slice_bits, bitstrings):
        c = lax.axis_index("cuts")
        m = lax.axis_index("grp")
        n0, _, ext = boundary.shape[:3]
        pair = ext * ext
        rows = gate_stack.shape[2]
        kdim = n0 * ext
        cols = pair // grps
        width = ext // cuts
        own_rows = rows // ext
        g = group_digits(bitstrings)
        count = bitstrings.shape[0]
        f32 = jnp.float32
        u32 = jnp.uint32
        order = layer_order.astype(u32)
        zero = u32(0)
        spot = m.astype(u32)

        gate0 = lax.dynamic_slice(gate_stack, (order[0], zero, zero, spot * u32(kdim)), (1, 2, rows, kdim))[0]
        big = jnp.stack((
            jnp.concatenate((gate0[0], -gate0[1]), axis=1),
            jnp.concatenate((gate0[1], gate0[0]), axis=1),
        ))
        big = big.reshape(2, own_rows, cuts, width, 2 * kdim)
        big = jnp.transpose(big, (2, 1, 0, 3, 4)).reshape(2 * rows, 2 * kdim)
        lh, ll = split(big)
        start = boundary.reshape(n0, 2, ext, pair)
        start = jnp.moveaxis(start, 1, 0).reshape(2 * kdim, pair)
        bh, bl = split(start)

        gate1 = lax.dynamic_slice(gate_stack, (order[1], zero, zero, spot * u32(cols)), (1, 2, rows, cols))[0]
        gate1 = jnp.transpose(gate1.reshape(2, own_rows, ext, cols), (2, 0, 1, 3))
        gate1 = gate1.reshape(ext, 2 * own_rows, cols)

        gate2 = lax.dynamic_slice(gate_stack, (order[2], zero, zero, zero), (1,) + gate_stack.shape[1:])[0]
        wanted = g[1] * ext + g[2] - rows * c
        pick = (wanted[:, None] == jnp.arange(rows)[None, :]).astype(f32)
        picked = lax.dot_general(pick, gate2, (((1,), (1,)), ((), ())), precision=HI)
        picked = picked.reshape(2, count // 2, 2, cuts, width, ext)
        picked = jnp.transpose(picked, (3, 1, 4, 0, 2, 5)).reshape(cuts, count // 2 * width, 4 * ext)

        column = m * cols + jnp.arange(cols, dtype=jnp.int32)
        span = jnp.arange(ext, dtype=jnp.int32)
        tile, lanes = 2 * width, 4 * ext
        wants = (
            (0, 7, g[0]), (1, 4, g[1]), (2, 4, g[2]), (3, 6, g[3]), (1, 3, span), (2, 2, span),
            (2, 1, column // ext), (3, 1, column % ext),
        )
        places = jnp.concatenate([place for _, _, place in wants])
        group_of = jnp.concatenate([jnp.full(p.shape, k, jnp.int32) for k, _, p in wants])
        layers_of = jnp.concatenate([jnp.full(p.shape, bits, jnp.int32) for _, bits, p in wants])
        layer, group, bit = (cut_index[:, k : k + 1] for k in range(3))
        active = (group == group_of[None]) & ((jnp.right_shift(layers_of[None], layer) & 1) == 1)
        agrees = (jnp.right_shift(places[None], bit) & 1) == slice_bits.reshape(-1, 1)
        kept = jnp.min(jnp.where(active & ~agrees, 0.0, 1.0), axis=0)
        pieces, at = [], 0
        for _, _, place in wants:
            pieces.append(kept[at : at + place.shape[0]][None])
            at += place.shape[0]
        last = pieces[0] * pieces[1] * pieces[2] * pieces[3]
        on_i1, on_i2 = pieces[4], pieces[5]
        on_j = pieces[6] * pieces[7]
        on_rows = jnp.tile(on_i1.reshape(cuts, width), (1, 2))
        on_rows = on_rows[:, :, None] * jnp.tile(on_i2, (1, 4))[None]
        on_b = jnp.pad(last, ((0, tile - 1), (0, lanes - count)))
        on_j = on_j.reshape(cols // lanes, lanes)
        on_j = jnp.pad(on_j, ((0, tile - on_j.shape[0]), (0, 0)))
        shared = jnp.broadcast_to(jnp.concatenate((on_b, on_j))[None], (cuts, 2 * tile, lanes))
        packed = jnp.concatenate((picked, on_rows, shared), axis=1)

        dma = pltpu.SemaphoreType.DMA
        smem = pl.BlockSpec(memory_space=pltpu.SMEM)
        small = (8, count)
        out = pl.pallas_call(
            functools.partial(whole_kernel, cuts, grps),
            out_shape=jax.ShapeDtypeStruct(small, f32),
            in_specs=[smem, smem] + [VMEM] * 6,
            out_specs=VMEM,
            scratch_shapes=[
                pltpu.VMEM((cuts,) + gate1.shape, f32),
                pltpu.VMEM((ext, tile, cols), f32),
                pltpu.VMEM((count // 4, 2, tile, lanes), f32),
                pltpu.VMEM((2, cuts, tile, lanes), f32),
                pltpu.VMEM((cuts, count, cols), f32),
                pltpu.VMEM((count, tile, cols), f32),
                pltpu.VMEM((grps - 1, 2 * rows, cols), f32),
                pltpu.VMEM((grps - 1, 2 * rows, cols), f32),
                pltpu.VMEM((cuts, own_rows, tile, cols), f32),
                pltpu.VMEM((cuts - 1,) + packed.shape[1:], f32),
                pltpu.VMEM((2, count, lanes), f32),
                pltpu.VMEM(small, f32), pltpu.VMEM((grps,) + small, f32),
                pltpu.VMEM(small, f32), pltpu.VMEM((cuts,) + small, f32),
                dma((10,)), dma((10,)), dma((grps - 1,)), dma((grps - 1,)),
                dma((cuts - 1,)), dma((cuts - 1,)), dma((cuts - 1,)), dma((cuts - 1,)), dma,
                dma((grps - 1,)), dma((grps - 1,)), dma((cuts - 1,)), dma((cuts - 1,)),
            ],
            compiler_params=pltpu.CompilerParams(
                collective_id=0, has_side_effects=True, vmem_limit_bytes=48 << 20
            ),
            name="whole",
        )(g[0], g[3], lh, ll, bh, bl, gate1, packed)
        return out[:2].T

    return body


def solution(mesh):
    fast = mesh.shape["cuts"] == 8 and mesh.shape["grp"] == 4
    maker = make_fast_body if fast else make_body
    return jax.shard_map(
        maker(mesh.shape["cuts"], mesh.shape["grp"]),
        mesh=mesh,
        in_specs=(
            P("grp", None, None, None, None),
            P(None, None, "cuts", None),
            P(),
            P(),
            P("cuts", None),
            P(),
        ),
        out_specs=P(),
        check_vma=False,
    )
```

```python
import functools

import jax
import jax.numpy as jnp
from jax import lax
from jax.experimental import pallas as pl
from jax.experimental.pallas import tpu as pltpu
from jax.sharding import PartitionSpec as P

LAYER_KINDS = (0, 1, 2, 3, 2, 3, 0, 1)
PAIR_GROUPS = ((0, 1), (2, 3), (1, 2), (1, 3))
PRECISION = lax.Precision.HIGH


def keep_mask(cut_index, slice_bits, layers, group_id, positions):
    hit = cut_index[:, 1] == group_id
    active = jnp.zeros_like(hit)
    for layer_id in layers:
        active = jnp.logical_or(active, cut_index[:, 0] == layer_id)
    active = jnp.logical_and(active, hit)
    bit_values = jnp.right_shift(positions[:, None], cut_index[None, :, 2]) & 1
    agrees = bit_values[None, :, :] == slice_bits[:, None, :]
    kept = jnp.logical_or(agrees, jnp.logical_not(active)[None, None, :])
    return jnp.all(kept, axis=2).astype(jnp.float32)


def group_digits(bitstrings):
    bits = bitstrings.shape[1] // 4
    weights = jnp.left_shift(jnp.ones((bits,), jnp.int32), jnp.arange(bits, dtype=jnp.int32))
    return [
        jnp.sum(bitstrings[:, k * bits : (k + 1) * bits] * weights, axis=1).astype(jnp.int32)
        for k in range(4)
    ]


def dot(a, b):
    return jnp.dot(a, b, precision=PRECISION, preferred_element_type=jnp.float32)


def make_body(cuts, grps):

    def body(boundary, gate_stack, layer_order, cut_index, slice_bits, bitstrings):
        c = lax.axis_index("cuts")
        m = lax.axis_index("grp")
        n0, _, ext = boundary.shape[:3]
        pair = ext * ext
        rows = gate_stack.shape[2]
        kdim = n0 * ext
        cols = pair // grps
        local_slices = slice_bits.shape[0]
        g = group_digits(bitstrings)
        count = bitstrings.shape[0]

        gate0 = lax.dynamic_index_in_dim(gate_stack, layer_order[0], 0, keepdims=False)
        gate0 = lax.dynamic_slice_in_dim(gate0, m * kdim, kdim, 2)
        start = jnp.moveaxis(boundary, 1, 0).reshape(2, kdim, pair)
        phi = jnp.stack((
            dot(gate0[0], start[0]) - dot(gate0[1], start[1]),
            dot(gate0[0], start[1]) + dot(gate0[1], start[0]),
        ))
        phi = lax.psum_scatter(phi, "grp", scatter_dimension=2, tiled=True)

        gate1 = lax.dynamic_index_in_dim(gate_stack, layer_order[1], 0, keepdims=False)
        gate1 = lax.dynamic_slice_in_dim(gate1, m * cols, cols, 2)
        gate1 = lax.all_gather(gate1, "cuts", axis=1, tiled=True)

        gate2 = lax.dynamic_index_in_dim(gate_stack, layer_order[2], 0, keepdims=False)
        wanted = g[1] * ext + g[2] - rows * c
        inside = jnp.logical_and(wanted >= 0, wanted < rows)
        picked = jnp.take(gate2, jnp.clip(wanted, 0, rows - 1), axis=1) * inside[None, :, None]
        if ext % cuts == 0:
            width, sub = ext // cuts, 1
            chunk = width * ext
            bits = jnp.zeros((2, cuts, local_slices, chunk), jnp.float32)
            bits = bits.at[:, :, :, : slice_bits.shape[1]].set(slice_bits.astype(jnp.float32))
            own = (jnp.arange(cuts) == c).astype(jnp.float32)
            bits = bits[:, :, None] * own[None, None, :, None, None]
            bits = bits.reshape(2, cuts, cuts * local_slices, chunk)
            bits = jnp.moveaxis(bits, 1, 2)
            packed = jnp.concatenate((picked.reshape(2, count, cuts, chunk), bits), axis=1)
            packed = lax.psum_scatter(packed, "cuts", scatter_dimension=2, tiled=True)[:, :, 0]
            gate2 = packed[:, :count].reshape(2, count, width, ext)
            slice_bits = packed[0, count:, : slice_bits.shape[1]].astype(jnp.int32)
            phi = phi.reshape(2, rows // ext, ext, cols)
            phi = lax.all_to_all(phi, "cuts", split_axis=2, concat_axis=1, tiled=True)
        else:
            width, sub = 1, cuts // ext
            slice_bits = lax.all_gather(slice_bits, "cuts", axis=0, tiled=True)
            picked = lax.psum(picked, "cuts").reshape(2, count, ext, ext)
            gate2 = lax.dynamic_slice_in_dim(picked, c // sub, 1, 2)
            phi = lax.all_gather(phi, "cuts", axis=1, tiled=True).reshape(2, ext, ext, cols)
            phi = lax.dynamic_slice_in_dim(phi, c // sub, 1, 2)
        first_i1 = c // sub * width
        cols = cols // sub
        first_col = (m * sub + c % sub) * cols
        if sub > 1:
            phi = lax.dynamic_slice_in_dim(phi, c % sub * cols, cols, 3)
            gate1 = lax.dynamic_slice_in_dim(gate1, c % sub * cols, cols, 2)

        slices = slice_bits.shape[0]
        column = first_col + jnp.arange(cols, dtype=jnp.int32)
        last = jnp.ones((slices, count), jnp.float32)
        for group_id, layers in ((0, (0, 1, 2)), (1, (2,)), (2, (2,)), (3, (1, 2))):
            last = last * keep_mask(cut_index, slice_bits, layers, group_id, g[group_id])
        on_i1 = keep_mask(
            cut_index, slice_bits, (0, 1), 1, first_i1 + jnp.arange(width, dtype=jnp.int32)
        )
        on_i2 = keep_mask(cut_index, slice_bits, (1,), 2, jnp.arange(ext, dtype=jnp.int32))
        on_j = keep_mask(cut_index, slice_bits, (0,), 2, column // ext)
        on_j = on_j * keep_mask(cut_index, slice_bits, (0,), 3, column % ext)

        left = gate2[:, :, None] * on_i2[None, None, :, None, :]
        left_re = jnp.concatenate((left[0], -left[1]), axis=3)
        left_im = jnp.concatenate((left[1], left[0]), axis=3)
        left = jnp.stack((left_re, left_im), axis=1)
        left = left.reshape(count, 2 * slices * width, 2 * ext)
        right = gate1.reshape(2, ext, ext, cols)
        right = jnp.take(jnp.moveaxis(right, 2, 0).reshape(ext, 2 * ext, cols), g[3], axis=0)
        w = lax.dot_general(
            left, right, (((2,), (1,)), ((0,), (0,))),
            precision=PRECISION, preferred_element_type=jnp.float32,
        )
        w = w.reshape(count, 2, slices, width, cols)
        scale = last.T[:, :, None, None] * on_i1[None, :, :, None] * on_j[None, :, None, :]
        w = jnp.sum(w * scale[:, None], axis=2)
        psi = jnp.take(phi, g[0], axis=1)
        real = jnp.sum(w[:, 0] * psi[0] - w[:, 1] * psi[1], axis=(1, 2))
        imag = jnp.sum(w[:, 0] * psi[1] + w[:, 1] * psi[0], axis=(1, 2))
        return lax.psum(jnp.stack((real, imag), axis=1), ("cuts", "grp"))

    return body


VMEM = pl.BlockSpec(memory_space=pltpu.VMEM)
HI = lax.Precision.HIGHEST


def split(x):
    hi = lax.reduce_precision(x, 8, 7)
    return hi.astype(jnp.bfloat16), (x - hi).astype(jnp.bfloat16)


def flip(index, step):
    return index + step * (1 - 2 * ((index // step) % 2))


def greet(cuts, grps):
    c, m = lax.axis_index("cuts"), lax.axis_index("grp")
    barrier = pltpu.get_barrier_semaphore()
    for d in range(1, cuts):
        pl.semaphore_signal(barrier, inc=1, device_id={"cuts": (c + d) % cuts})
    for d in range(1, grps):
        pl.semaphore_signal(barrier, inc=1, device_id={"grp": (m + d) % grps})
    pl.semaphore_wait(barrier, cuts + grps - 2)
    return c, m


def whole_kernel(
    cuts, grps, g0, g3, lh, ll, bh, bl, u1, packed, out,
    u1_all, phi, base, masks, weight, wt,
    parts, landed, phis, u2_in, acc, mine, from_grp, mid, from_cuts,
    u_send, u_recv, r_send, r_recv, p_send, p_recv, k_send, k_recv, own_sem,
    g_send, g_recv, c_send, c_recv,
):
    c, m = greet(cuts, grps)
    core, east, north = flip(c, 1), flip(c, 2), flip(c, 4)
    half = u1.shape[0] // 2
    low, high = pl.ds(0, half), pl.ds(half, half)

    def send_u1(slot, src, dst, target):
        return pltpu.make_async_remote_copy(
            src_ref=src, dst_ref=dst, send_sem=u_send.at[slot], recv_sem=u_recv.at[slot],
            device_id={"cuts": target},
        )

    own = pltpu.make_async_copy(u1, u1_all.at[c], own_sem)
    own.start()
    east_low = send_u1(0, u1.at[low], u1_all.at[c, low], east)
    north_high = send_u1(1, u1.at[high], u1_all.at[c, high], north)
    east_high = send_u1(2, u1.at[high], u1_all.at[c, high], east)
    north_low = send_u1(3, u1.at[low], u1_all.at[c, low], north)
    to_core = send_u1(4, u1, u1_all.at[c], core)
    for copy in (east_low, north_high, east_high, north_low, to_core):
        copy.start()

    row_copies = []
    for d in range(1, cuts):
        to = (c + d) % cuts
        copy = pltpu.make_async_remote_copy(
            src_ref=packed.at[to], dst_ref=u2_in.at[d - 1],
            send_sem=k_send.at[d - 1], recv_sem=k_recv.at[d - 1], device_id={"cuts": to},
        )
        row_copies.append(copy)

    cols = parts.shape[2]

    def product(part):
        at = pl.ds(pl.multiple_of(part * cols, cols), cols)
        bhi, blo = bh[:, at], bl[:, at]
        mm = functools.partial(jnp.dot, preferred_element_type=jnp.float32)
        return mm(lh[...], bhi) + (mm(lh[...], blo) + mm(ll[...], bhi))

    near, across = flip(m, 1), flip(m, 2)

    def send_sum(slot, target):
        return pltpu.make_async_remote_copy(
            src_ref=parts.at[slot], dst_ref=landed.at[slot],
            send_sem=r_send.at[slot], recv_sem=r_recv.at[slot], device_id={"grp": target},
        )

    sums = [send_sum(0, near), send_sum(1, near), send_sum(2, across)]
    parts[0] = product(flip(near, 2))
    sums[0].start()
    parts[1] = product(near)
    sums[1].start()
    carried = product(across)
    total = product(m)

    east_low.wait_recv()
    on_north = send_u1(5, u1_all.at[east, low], u1_all.at[east, low], north)
    on_north.start()
    north_high.wait_recv()
    on_east = send_u1(6, u1_all.at[north, high], u1_all.at[north, high], east)
    on_east.start()
    for copy in row_copies:
        copy.start()
    sums[0].wait_recv()
    parts[2] = carried + landed[0]
    sums[2].start()
    east_high.wait_recv()
    core_east = send_u1(7, u1_all.at[east], u1_all.at[east], core)
    core_east.start()
    north_low.wait_recv()
    core_north = send_u1(8, u1_all.at[north], u1_all.at[north], core)
    core_north.start()
    on_north.wait_recv()
    on_east.wait_recv()
    far = flip(east, 4)
    core_far = send_u1(9, u1_all.at[far], u1_all.at[far], core)
    core_far.start()


    lanes = packed.shape[2]
    tile = phi.shape[1]
    half_tile = tile // 2
    count = wt.shape[0]
    pairs = count // 2
    picked_rows = pairs * half_tile
    for d in range(1, cuts):
        row_copies[d - 1].wait_recv()
    rows = packed[c, pl.ds(0, picked_rows)]
    for d in range(1, cuts):
        rows = rows + u2_in[d - 1, pl.ds(0, picked_rows)]
    rows = rows.reshape(picked_rows // tile, tile, lanes)
    lane = lax.broadcasted_iota(jnp.int32, (1, 1, lanes), 2)
    row = lax.broadcasted_iota(jnp.int32, (1, tile, 1), 1)
    quarter = lanes // 4
    even = (lane // quarter) % 2 == 0
    real_rows = jnp.where(even, rows, -rows)
    imag_rows = jnp.where(even, pltpu.roll(rows, lanes - quarter, 2), pltpu.roll(rows, quarter, 2))
    upper = row < half_tile
    base[:, 0] = jnp.where(upper, real_rows, pltpu.roll(imag_rows, half_tile, 1))
    base[:, 1] = jnp.where(upper, pltpu.roll(real_rows, half_tile, 1), imag_rows)
    first = lax.broadcasted_iota(jnp.int32, (1, lanes), 1) < lanes // 2
    for s in range(cuts):
        slot = packed.at[c] if s == 0 else u2_in.at[s - 1]
        mask = slot[pl.ds(picked_rows, tile)]
        masks[0, s] = jnp.where(first, mask, 0.0)
        masks[1, s] = jnp.where(first, 0.0, mask)
        on_b = slot[pl.ds(picked_rows + tile, tile)]
        on_j = slot[pl.ds(picked_rows + 2 * tile, tile)]
        column = jnp.transpose(on_b)[:count, 0:1]
        weight[s] = column * jnp.concatenate(
            [on_j[k : k + 1] for k in range(weight.shape[2] // lanes)], axis=1
        )

    for copy in (to_core, core_east, core_north, core_far):
        copy.wait_recv()
    own.wait()

    def block_of(b):
        block = u1_all[:, g3[b]]
        block = block.reshape(cuts // 2, 2, tile, block.shape[2])
        one, two = block[:, 0], block[:, 1]
        one_t, two_t = pltpu.roll(one, half_tile, 1), pltpu.roll(two, half_tile, 1)
        re, im = jnp.where(upper, one, two_t), jnp.where(upper, one_t, two)
        both = jnp.concatenate((re, im), axis=0)
        return both.reshape(cuts * tile, both.shape[2])

    def in_two(x):
        hi = x.astype(jnp.bfloat16)
        return hi, (x - hi.astype(jnp.float32)).astype(jnp.bfloat16)

    mm = functools.partial(jnp.dot, preferred_element_type=jnp.float32)

    def apply_rows(p, carry):
        right = jnp.concatenate((block_of(p), block_of(p + pairs)), axis=0)
        rhi, rlo = in_two(right)
        left = base[p // 2, p % 2][None, None] * masks[...]
        lhi, llo = in_two(left.reshape(2 * cuts * tile, lanes))
        w = mm(lhi, rhi) + (mm(lhi, rlo) + mm(llo, rhi))
        w = w.reshape(2, cuts, tile, w.shape[1])
        for h in range(2):
            at = p + h * pairs
            wt[at] = jnp.sum(w[h] * weight[:, pl.ds(at, 1), :], axis=0)
        return carry

    lax.fori_loop(0, pairs, apply_rows, 0, unroll=2)

    for slot in (1, 2):
        sums[slot].wait_recv()
        total = total + landed[slot]
    phis[...] = total.reshape(phis.shape)
    own_rows = phis.shape[1]
    place = pl.ds(c * own_rows, own_rows)
    phi[place] = phis[c]
    turned = []
    for d in range(1, cuts):
        to = (c + d) % cuts
        copy = pltpu.make_async_remote_copy(
            src_ref=phis.at[to], dst_ref=phi.at[place],
            send_sem=p_send.at[d - 1], recv_sem=p_recv.at[d - 1], device_id={"cuts": to},
        )
        copy.start()
        turned.append(copy)
    for copy in turned:
        copy.wait_recv()

    sign = jnp.where(lax.broadcasted_iota(jnp.int32, (tile, 1), 0) < half_tile, 1.0, -1.0)

    def fold(v):
        return functools.reduce(
            lambda p, q: p + q, [v[:, k : k + lanes] for k in range(0, v.shape[1], lanes)]
        )

    def one(b, carry):
        psi = phi[g0[b]]
        w = wt[b]
        swapped = pltpu.roll(psi, half_tile, 0)
        acc[0, pl.ds(b, 1), :] = jnp.sum(fold(w * psi) * sign, axis=0, keepdims=True)
        acc[1, pl.ds(b, 1), :] = jnp.sum(fold(w * swapped), axis=0, keepdims=True)
        return carry

    lax.fori_loop(0, count, one, 0, unroll=4)
    ones = jnp.ones((8, lanes), jnp.float32)
    add = lambda v: lax.dot_general(
        ones, v, (((1,), (1,)), ((), ())), precision=HI, preferred_element_type=jnp.float32
    )
    mine[...] = jnp.where(
        lax.broadcasted_iota(jnp.int32, mine.shape, 0) == 0, add(acc[0]), add(acc[1])
    )

    def everyone(axis, me, size, src, slots, send, recv):
        slots[me] = src[...]
        copies = []
        for d in range(1, size):
            to = (me + d) % size
            copy = pltpu.make_async_remote_copy(
                src_ref=src, dst_ref=slots.at[me],
                send_sem=send.at[d - 1], recv_sem=recv.at[d - 1], device_id={axis: to},
            )
            copy.start()
            copies.append(copy)
        for copy in copies:
            copy.wait()
        return functools.reduce(lambda p, q: p + q, [slots[k] for k in range(size)])

    mid[...] = everyone("grp", m, grps, mine, from_grp, g_send, g_recv)
    out[...] = everyone("cuts", c, cuts, mid, from_cuts, c_send, c_recv)
    for copy in (
        east_low, north_high, east_high, north_low, to_core, on_north, on_east,
        core_east, core_north, core_far, *row_copies, *sums, *turned,
    ):
        copy.wait_send()


def make_fast_body(cuts, grps):

    def body(boundary, gate_stack, layer_order, cut_index, slice_bits, bitstrings):
        c = lax.axis_index("cuts")
        m = lax.axis_index("grp")
        n0, _, ext = boundary.shape[:3]
        pair = ext * ext
        rows = gate_stack.shape[2]
        kdim = n0 * ext
        cols = pair // grps
        width = ext // cuts
        own_rows = rows // ext
        g = group_digits(bitstrings)
        count = bitstrings.shape[0]
        f32 = jnp.float32
        u32 = jnp.uint32
        order = layer_order.astype(u32)
        zero = u32(0)
        spot = m.astype(u32)

        gate0 = lax.dynamic_slice(gate_stack, (order[0], zero, zero, spot * u32(kdim)), (1, 2, rows, kdim))[0]
        big = jnp.stack((
            jnp.concatenate((gate0[0], -gate0[1]), axis=1),
            jnp.concatenate((gate0[1], gate0[0]), axis=1),
        ))
        big = big.reshape(2, own_rows, cuts, width, 2 * kdim)
        big = jnp.transpose(big, (2, 1, 0, 3, 4)).reshape(2 * rows, 2 * kdim)
        lh, ll = split(big)
        start = boundary.reshape(n0, 2, ext, pair)
        start = jnp.moveaxis(start, 1, 0).reshape(2 * kdim, pair)
        bh, bl = split(start)

        gate1 = lax.dynamic_slice(gate_stack, (order[1], zero, zero, spot * u32(cols)), (1, 2, rows, cols))[0]
        gate1 = jnp.transpose(gate1.reshape(2, own_rows, ext, cols), (2, 0, 1, 3))
        gate1 = gate1.reshape(ext, 2 * own_rows, cols)

        gate2 = lax.dynamic_slice(gate_stack, (order[2], zero, zero, zero), (1,) + gate_stack.shape[1:])[0]
        wanted = g[1] * ext + g[2] - rows * c
        pick = (wanted[:, None] == jnp.arange(rows)[None, :]).astype(f32)
        picked = lax.dot_general(pick, gate2, (((1,), (1,)), ((), ())), precision=HI)
        picked = picked.reshape(2, count // 2, 2, cuts, width, ext)
        picked = jnp.transpose(picked, (3, 1, 4, 0, 2, 5)).reshape(cuts, count // 2 * width, 4 * ext)

        column = m * cols + jnp.arange(cols, dtype=jnp.int32)
        span = jnp.arange(ext, dtype=jnp.int32)
        tile, lanes = 2 * width, 4 * ext
        wants = (
            (0, 7, g[0]), (1, 4, g[1]), (2, 4, g[2]), (3, 6, g[3]), (1, 3, span), (2, 2, span),
            (2, 1, column // ext), (3, 1, column % ext),
        )
        places = jnp.concatenate([place for _, _, place in wants])
        group_of = jnp.concatenate([jnp.full(p.shape, k, jnp.int32) for k, _, p in wants])
        layers_of = jnp.concatenate([jnp.full(p.shape, bits, jnp.int32) for _, bits, p in wants])
        layer, group, bit = (cut_index[:, k : k + 1] for k in range(3))
        active = (group == group_of[None]) & ((jnp.right_shift(layers_of[None], layer) & 1) == 1)
        agrees = (jnp.right_shift(places[None], bit) & 1) == slice_bits.reshape(-1, 1)
        kept = jnp.min(jnp.where(active & ~agrees, 0.0, 1.0), axis=0)
        pieces, at = [], 0
        for _, _, place in wants:
            pieces.append(kept[at : at + place.shape[0]][None])
            at += place.shape[0]
        last = pieces[0] * pieces[1] * pieces[2] * pieces[3]
        on_i1, on_i2 = pieces[4], pieces[5]
        on_j = pieces[6] * pieces[7]
        on_rows = jnp.tile(on_i1.reshape(cuts, width), (1, 2))
        on_rows = on_rows[:, :, None] * jnp.tile(on_i2, (1, 4))[None]
        on_b = jnp.pad(last, ((0, tile - 1), (0, lanes - count)))
        on_j = on_j.reshape(cols // lanes, lanes)
        on_j = jnp.pad(on_j, ((0, tile - on_j.shape[0]), (0, 0)))
        shared = jnp.broadcast_to(jnp.concatenate((on_b, on_j))[None], (cuts, 2 * tile, lanes))
        packed = jnp.concatenate((picked, on_rows, shared), axis=1)

        dma = pltpu.SemaphoreType.DMA
        smem = pl.BlockSpec(memory_space=pltpu.SMEM)
        small = (8, count)
        out = pl.pallas_call(
            functools.partial(whole_kernel, cuts, grps),
            out_shape=jax.ShapeDtypeStruct(small, f32),
            in_specs=[smem, smem] + [VMEM] * 6,
            out_specs=VMEM,
            scratch_shapes=[
                pltpu.VMEM((cuts,) + gate1.shape, f32),
                pltpu.VMEM((ext, tile, cols), f32),
                pltpu.VMEM((count // 4, 2, tile, lanes), f32),
                pltpu.VMEM((2, cuts, tile, lanes), f32),
                pltpu.VMEM((cuts, count, cols), f32),
                pltpu.VMEM((count, tile, cols), f32),
                pltpu.VMEM((grps - 1, 2 * rows, cols), f32),
                pltpu.VMEM((grps - 1, 2 * rows, cols), f32),
                pltpu.VMEM((cuts, own_rows, tile, cols), f32),
                pltpu.VMEM((cuts - 1,) + packed.shape[1:], f32),
                pltpu.VMEM((2, count, lanes), f32),
                pltpu.VMEM(small, f32), pltpu.VMEM((grps,) + small, f32),
                pltpu.VMEM(small, f32), pltpu.VMEM((cuts,) + small, f32),
                dma((10,)), dma((10,)), dma((grps - 1,)), dma((grps - 1,)),
                dma((cuts - 1,)), dma((cuts - 1,)), dma((cuts - 1,)), dma((cuts - 1,)), dma,
                dma((grps - 1,)), dma((grps - 1,)), dma((cuts - 1,)), dma((cuts - 1,)),
            ],
            compiler_params=pltpu.CompilerParams(
                collective_id=0, has_side_effects=True, vmem_limit_bytes=48 << 20
            ),
            name="whole",
        )(g[0], g[3], lh, ll, bh, bl, gate1, packed)
        return out[:2].T

    return body


def solution(mesh):
    fast = mesh.shape["cuts"] == 8 and mesh.shape["grp"] == 4
    maker = make_fast_body if fast else make_body
    return jax.shard_map(
        maker(mesh.shape["cuts"], mesh.shape["grp"]),
        mesh=mesh,
        in_specs=(
            P("grp", None, None, None, None),
            P(None, None, "cuts", None),
            P(),
            P(),
            P("cuts", None),
            P(),
        ),
        out_specs=P(),
        check_vma=False,
    )
```
